128 devices in a mesh: row: 16 (over y, x), col: 8 (over z, core).
Axes of the slice: x: 4, y: 4, z: 4, core: 2. Of those that a mesh axis runs over, the one named last changes fastest.
Arguments:
- tangents: float32 [192, 128, 6144], P('row', None, 'col'), may hold values from -6 to 6
- base_flow: float32 [192, 128, 192], P('row', None, 'col'), may hold values from -0.0625 to 0.0625
- mode_mask: int32 [192, 192], P('row', 'col'), may hold values 0 or 1
- decay_rates: float32 [128], replicated, may hold values from 1 to 100
- to_eigen: float32 [128, 128], replicated, may hold values from -0.5 to 0.5
- from_eigen: float32 [128, 128], replicated, may hold values from -0.5 to 0.5
Outputs:
- vectors: float32 [192, 128, 6144], P('row', None, 'col')
- growth: float32 [32], replicated
The draws below stay inside these ranges and needn't reach their ends.
Inputs may be any that keep to these rules, and one draw needn't show every extreme that they name: `mode_mask`: 1 keeps a mode pair of the linearized product, 0 removes it.
All inputs are finite; a program needn't handle non-finite values. No bound on the sum of `mode_mask` on one device may be relied on, other than what follows from the above.
Results may differ from the reference program's by a relative error of at most 0.00005.
Values sent between devices are 32-bit elements; how exact they have to be, the bound alone decides.
A program may use at most 128 MiB of HBM per device.

```python
import math
import jax
import jax.numpy as jnp
from jax import lax

NX = 192
NY = 128
NZ = 192
NV = 32


def plant(values, rng, least, top_value):
    longest = values.shape.index(max(values.shape))
    spots = []
    for shift in (0, 1):
        where = [jax.random.randint(jax.random.fold_in(rng, axis), (), 0, length) for axis, length in enumerate(values.shape)]
        where[longest] = (where[longest] + shift) % values.shape[longest]
        spots.append(tuple(where))
    return values.at[spots[0]].set(least).at[spots[1]].set(top_value)


def block_scale(rng, shape, pieces, least, high):
    factor_of, own = 1.0, jax.random.fold_in(rng, 6)
    for axis_at, parts in pieces:
        heights = jnp.exp(jax.random.uniform(jax.random.fold_in(own, axis_at), (parts,), jnp.float32, least / len(pieces), high / len(pieces)))
        factor_of = factor_of * jnp.repeat(heights, shape[axis_at] // parts).reshape([-1 if axis == axis_at else 1 for axis in range(len(shape))])
    return factor_of


def centred(rng, dims, deviation, most, cuts=(), kind=jnp.bfloat16):
    drawn = deviation * jax.random.normal(rng, dims, jnp.float32)
    if cuts:
        drawn = drawn * block_scale(rng, dims, cuts, -0.22, 0.18)
    return jnp.clip(drawn, -most, most).astype(kind)


def setup_inputs(seed: int = 0) -> dict:
    key_list = jax.random.split(jax.random.key(seed), 7)
    tangents = centred(key_list[0], (NX, NY, NZ * NV), 1.0, 6.0, ((0, 16), (2, 8)), jnp.float32)
    base_flow = centred(key_list[1], (NX, NY, NZ), (NX * NZ // 4) ** -0.5, 0.0625, ((0, 16), (2, 8)), jnp.float32)
    mode_mask = plant((jax.random.randint(key_list[2], (NX, NZ), 0, 4) < 3).astype(jnp.int32), jax.random.fold_in(key_list[2], 1), 0, 1)
    decay_rates = jnp.clip(jnp.exp(jax.random.uniform(key_list[3], (NY,), jnp.float32, math.log(1.0), math.log(100.0))), 1.0, 100.0)
    to_eigen = centred(key_list[4], (NY, NY), NY ** -0.5, 0.5, (), jnp.float32)
    from_eigen = centred(key_list[5], (NY, NY), NY ** -0.5, 0.5, (), jnp.float32)
    return dict(tangents=tangents, base_flow=base_flow, mode_mask=mode_mask, decay_rates=decay_rates, to_eigen=to_eigen, from_eigen=from_eigen)


PRECISE = lax.Precision.HIGHEST
STEP_COEF = 10.0
VISCOSITY = 0.01
ALPHA_X = 0.5
BETA_Z = 1.0

def local_waves(points_count, first_index, length):
    indices = first_index + jnp.arange(length, dtype=jnp.int32)
    middle = points_count // 2
    return jnp.where(indices <= middle, indices, indices - middle).astype(jnp.float32)

def synthesis(points_count):
    points = jnp.arange(points_count, dtype=jnp.int32)[:, None]
    mode_index = jnp.arange(points_count, dtype=jnp.int32)[None, :]
    middle = points_count // 2
    wave_index = jnp.where(mode_index <= middle, mode_index, mode_index - middle)
    turn_count = (points * wave_index % points_count).astype(jnp.float32)
    angles = turn_count * (2.0 * math.pi / points_count)
    return jnp.where(mode_index <= middle, jnp.cos(angles), jnp.sin(angles))

def analysis(points_count):
    mode_index = jnp.arange(points_count, dtype=jnp.int32)
    middle = points_count // 2
    weights = jnp.where((mode_index == 0) | (mode_index == middle), jnp.float32(1.0 / points_count), jnp.float32(2.0 / points_count))
    return weights[:, None] * synthesis(points_count).T

def derivative_analysis(points_count, wave_scale):
    rows_index = jnp.arange(points_count, dtype=jnp.int32)[:, None]
    cols_index = jnp.arange(points_count, dtype=jnp.int32)[None, :]
    middle = points_count // 2
    rising = (cols_index == rows_index + middle) & (rows_index >= 1) & (rows_index < middle)
    falling = (rows_index == cols_index + middle) & (cols_index >= 1) & (cols_index < middle)
    rows_float = jnp.broadcast_to(rows_index.astype(jnp.float32), (points_count, points_count))
    cols_float = jnp.broadcast_to(cols_index.astype(jnp.float32), (points_count, points_count))
    derivative = jnp.where(rising, rows_float, jnp.float32(0.0)) - jnp.where(falling, cols_float, jnp.float32(0.0))
    return -wave_scale * jnp.dot(derivative, analysis(points_count), precision=PRECISE)

def denominators(decay_rates, x_count, z_count, x_start, z_start, x_length, z_length):
    wave_x = ALPHA_X * local_waves(x_count, x_start, x_length)
    wave_z = BETA_Z * local_waves(z_count, z_start, z_length)
    return STEP_COEF + VISCOSITY * (wave_x[:, None, None] ** 2 + wave_z[None, None, :] ** 2) + decay_rates[None, :, None]

def reference(tangents, base_flow, mode_mask, decay_rates, to_eigen, from_eigen):
    x_count, y_count, z_count = base_flow.shape
    vec_count = tangents.shape[2] // z_count
    fields = jnp.transpose(tangents.reshape(x_count, y_count, z_count, vec_count), (3, 0, 1, 2))
    x_synthesis = synthesis(x_count)
    z_synthesis = synthesis(z_count)
    x_derivative = derivative_analysis(x_count, ALPHA_X)
    z_analysis = analysis(z_count)
    speed_field = jnp.einsum('pm,myn->pyn', x_synthesis, base_flow, precision=PRECISE)
    speed_field = jnp.einsum('pyn,sn->pys', speed_field, z_synthesis, precision=PRECISE)
    divisor = denominators(decay_rates, x_count, z_count, 0, 0, x_count, z_count)
    retained = mode_mask.astype(jnp.float32)[:, None, :]

    def advance(one_field):
        physical = jnp.einsum('pm,myn->pyn', x_synthesis, one_field, precision=PRECISE)
        physical = jnp.einsum('pyn,sn->pys', physical, z_synthesis, precision=PRECISE)
        product = speed_field * physical
        returned = jnp.einsum('mp,pys->mys', x_derivative, product, precision=PRECISE)
        returned = jnp.einsum('mys,ns->myn', returned, z_analysis, precision=PRECISE)
        right_side = STEP_COEF * one_field + retained * returned
        eigen_part = jnp.einsum('ji,min->mjn', to_eigen, right_side, precision=PRECISE) / divisor
        return jnp.einsum('yj,mjn->myn', from_eigen, eigen_part, precision=PRECISE)
    stepped = lax.map(advance, fields)
    cell_count = x_count * y_count * z_count
    gram_matrix = jnp.einsum('vmyn,umyn->vu', stepped, stepped, precision=PRECISE) / cell_count
    lower_factor = jnp.linalg.cholesky(gram_matrix)
    identity = jnp.eye(vec_count, dtype=jnp.float32)
    inverse = jax.scipy.linalg.solve_triangular(lower_factor, identity, lower=True)
    orthonormal = jnp.einsum('uv,vmyn->mynu', inverse, stepped, precision=PRECISE)
    growth = jnp.log(jnp.diagonal(lower_factor))
    return (orthonormal.reshape(x_count, y_count, z_count * vec_count), growth)
```

```python
import math

import jax
import jax.numpy as jnp
from jax import lax
from jax.experimental import pallas as pl
from jax.experimental.pallas import tpu as pltpu
from jax.sharding import PartitionSpec as P

PRECISE = lax.Precision.HIGHEST
STEP_COEF = 10.0
VISCOSITY = 0.01
ALPHA_X = 0.5
BETA_Z = 1.0


def side_by_side(arrays, axis, split_dim, concat_dim, along):
    widths = [a.shape[along] for a in arrays]
    both = jnp.concatenate(arrays, axis=along)
    out = lax.all_to_all(both, axis, split_axis=split_dim, concat_axis=concat_dim, tiled=True)
    return tuple(jnp.split(out, [sum(widths[:k]) for k in range(1, len(widths))], axis=along))


def swap_kernel(x_ref, o_ref, ss, rs, ls):
    r = lax.axis_index("row")
    c = lax.axis_index("col")
    me = r * 8 + c
    own = pltpu.make_async_copy(x_ref.at[me], o_ref.at[me], ls)
    own.start()

    def send(k, carry):
        off = lax.rem(k * 37, 128)
        r2 = lax.rem(r + off // 8, 16)
        c2 = lax.rem(c + lax.rem(off, 8), 8)
        pltpu.make_async_remote_copy(
            x_ref.at[r2 * 8 + c2], o_ref.at[me], ss, rs,
            device_id=(r2, c2), device_id_type=pl.DeviceIdType.MESH,
        ).start()
        return carry

    lax.fori_loop(1, 128, send, 0)
    own.wait()
    pltpu.make_async_copy(x_ref.at[pl.ds(0, 127)], o_ref.at[pl.ds(0, 127)], rs).wait()
    pltpu.make_async_copy(x_ref.at[pl.ds(0, 127)], o_ref.at[pl.ds(0, 127)], ss).wait()


def swap(x):
    return pl.pallas_call(
        swap_kernel,
        out_shape=jax.ShapeDtypeStruct(x.shape, x.dtype),
        in_specs=[pl.BlockSpec(memory_space=pl.ANY)],
        out_specs=pl.BlockSpec(memory_space=pl.ANY),
        scratch_shapes=[pltpu.SemaphoreType.DMA] * 3,
        compiler_params=pltpu.CompilerParams(has_side_effects=True),
    )(x)


def total_of_pieces(shard, axis):
    return lax.all_gather(shard, axis).sum(0)


def local_waves(points_count, first_index, length):
    indices = first_index + jnp.arange(length, dtype=jnp.int32)
    middle = points_count // 2
    return jnp.where(indices <= middle, indices, indices - middle).astype(jnp.float32)


def synthesis(points_count):
    points = jnp.arange(points_count, dtype=jnp.int32)[:, None]
    mode_index = jnp.arange(points_count, dtype=jnp.int32)[None, :]
    middle = points_count // 2
    wave_index = jnp.where(mode_index <= middle, mode_index, mode_index - middle)
    turn_count = (points * wave_index % points_count).astype(jnp.float32)
    angles = turn_count * (2.0 * math.pi / points_count)
    return jnp.where(mode_index <= middle, jnp.cos(angles), jnp.sin(angles))


def analysis(points_count):
    mode_index = jnp.arange(points_count, dtype=jnp.int32)
    middle = points_count // 2
    weights = jnp.where(
        (mode_index == 0) | (mode_index == middle),
        jnp.float32(1.0 / points_count),
        jnp.float32(2.0 / points_count),
    )
    return weights[:, None] * synthesis(points_count).T


def derivative_analysis(points_count, wave_scale):
    rows_index = jnp.arange(points_count, dtype=jnp.int32)[:, None]
    cols_index = jnp.arange(points_count, dtype=jnp.int32)[None, :]
    middle = points_count // 2
    rising = (cols_index == rows_index + middle) & (rows_index >= 1) & (rows_index < middle)
    falling = (rows_index == cols_index + middle) & (cols_index >= 1) & (cols_index < middle)
    rows_float = jnp.broadcast_to(rows_index.astype(jnp.float32), (points_count, points_count))
    cols_float = jnp.broadcast_to(cols_index.astype(jnp.float32), (points_count, points_count))
    derivative = jnp.where(rising, rows_float, jnp.float32(0.0)) - jnp.where(
        falling, cols_float, jnp.float32(0.0)
    )
    return -wave_scale * jnp.dot(derivative, analysis(points_count), precision=PRECISE)


def denominators(decay_rates, x_count, z_count, x_start, z_start, x_length, z_length):
    wave_x = ALPHA_X * local_waves(x_count, x_start, x_length)
    wave_z = BETA_Z * local_waves(z_count, z_start, z_length)
    return (
        STEP_COEF
        + VISCOSITY * (wave_x[:, None, None] ** 2 + wave_z[None, None, :] ** 2)
        + decay_rates[None, :, None]
    )


def body(tangents, base_flow, mode_mask, decay_rates, to_eigen, from_eigen):
    x_length, y_count, zv_length = tangents.shape
    z_length = base_flow.shape[2]
    vec_count = zv_length // z_length
    row_devices = lax.axis_size("row")
    col_devices = lax.axis_size("col")
    x_count = x_length * row_devices
    z_count = z_length * col_devices
    x_synthesis = synthesis(x_count)
    z_synthesis = synthesis(z_count)
    x_derivative = derivative_analysis(x_count, ALPHA_X)
    z_analysis = analysis(z_count)
    all_devices = row_devices * col_devices
    plane_count = y_count // all_devices
    stacked = tangents.reshape(x_length, y_count, 1, zv_length)
    speed_stack = base_flow.reshape(x_length, y_count, 1, z_length)
    speed_field = lax.all_to_all(speed_stack, ("row", "col"), split_axis=1, concat_axis=2, tiled=True)
    pieces = jnp.transpose(tangents, (1, 0, 2)).reshape(y_count, x_length * zv_length // 128, 128)
    planes = swap(pieces).reshape(1, all_devices, x_length, zv_length)
    planes = jnp.transpose(planes, (2, 0, 1, 3))
    x_table = x_synthesis.reshape(x_count, row_devices, x_length)
    z_table = z_synthesis.reshape(z_count, col_devices, z_length)
    planes = planes.reshape(x_length, plane_count, row_devices, col_devices, z_length, vec_count)
    physical = jnp.einsum("myrcnv,prm->ypcnv", planes, x_table, precision=PRECISE)
    physical = jnp.einsum("ypcnv,scn->ypsv", physical, z_table, precision=PRECISE)
    speed_field = speed_field.reshape(x_length, plane_count, row_devices, col_devices, z_length)
    speed_field = jnp.einsum("myrcn,prm->ypcn", speed_field, x_table, precision=PRECISE)
    speed_field = jnp.einsum("ypcn,scn->yps", speed_field, z_table, precision=PRECISE)
    product = physical * speed_field[:, :, :, None]
    returned = jnp.einsum("ypsv,ns->ypnv", product, z_analysis, precision=PRECISE)
    returned = jnp.einsum("ypnv,mp->ymnv", returned, x_derivative, precision=PRECISE)
    returned = returned.reshape(
        plane_count, row_devices, x_length, col_devices, z_length, vec_count
    )
    returned = jnp.transpose(returned, (2, 0, 1, 3, 4, 5)).reshape(
        x_length, plane_count, all_devices, zv_length
    )
    nonlinear = lax.all_to_all(returned, ("row", "col"), split_axis=2, concat_axis=1, tiled=True)
    nonlinear = nonlinear.reshape(x_length, y_count, zv_length)
    x_start = lax.axis_index("row") * x_length
    z_start = lax.axis_index("col") * z_length
    divisor = denominators(decay_rates, x_count, z_count, x_start, z_start, x_length, z_length)
    retained = mode_mask.astype(jnp.float32)[:, None, :, None]
    nonlinear = nonlinear.reshape(x_length, y_count, z_length, vec_count) * retained
    right_side = STEP_COEF * tangents.reshape(x_length, y_count, z_length, vec_count) + nonlinear
    eigen_part = jnp.einsum(
        "ji,mic->mjc", to_eigen, right_side.reshape(x_length, y_count, zv_length), precision=PRECISE
    )
    eigen_part = eigen_part.reshape(x_length, y_count, z_length, vec_count) / divisor[:, :, :, None]
    stepped = jnp.einsum(
        "yj,mjc->myc",
        from_eigen,
        eigen_part.reshape(x_length, y_count, zv_length),
        precision=PRECISE,
    )
    columns = stepped.reshape(x_length * y_count * z_length, vec_count)
    cell_count = x_count * y_count * z_count
    identity = jnp.eye(vec_count, dtype=jnp.float32)
    local_gram = jnp.einsum("cv,cu->vu", columns, columns, precision=PRECISE)
    gram_matrix = total_of_pieces(local_gram, ("row", "col")) / cell_count
    lower_factor = jnp.linalg.cholesky(gram_matrix)
    inverse = jax.scipy.linalg.solve_triangular(lower_factor, identity, lower=True)
    orthonormal = jnp.einsum("cv,uv->cu", columns, inverse, precision=PRECISE)
    growth = jnp.log(jnp.diagonal(lower_factor))
    return (orthonormal.reshape(x_length, y_count, zv_length), growth)


def solution(mesh):
    placed = (P("row", None, "col"), P("row", None, "col"), P("row", "col"), P(), P(), P())
    return jax.shard_map(
        body, mesh=mesh, in_specs=placed, out_specs=(P("row", None, "col"), P()), check_vma=False
    )
```

```python
import functools
import math

import jax
import jax.numpy as jnp
import numpy as np
from jax import lax
from jax.experimental import pallas as pl
from jax.experimental.pallas import tpu as pltpu
from jax.sharding import PartitionSpec as P

MESH = pl.DeviceIdType.MESH
F32 = jnp.float32
BF16 = jnp.bfloat16
STEP_COEF = 10.0
VISCOSITY = 0.01
ALPHA_X = 0.5
BETA_Z = 1.0

NX = 192
NY = 128
NZ = 192
NV = 32
NR, NC = 16, 8
ND = NR * NC
ML = NX // NR
LANES = 128
LO = LANES // NV
HI = NZ // LO
NH = HI // NC
PIECE = ML * NH
BASE = ML // LO
HOP = 37


def synthesis(n):
    point = np.arange(n)[:, None]
    mode = np.arange(n)[None, :]
    wave = np.where(mode <= n // 2, mode, mode - n // 2)
    angle = (point * wave % n) * (2.0 * math.pi / n)
    return np.where(mode <= n // 2, np.cos(angle), np.sin(angle))


def analysis(n):
    mode = np.arange(n)
    weight = np.where((mode == 0) | (mode == n // 2), 1.0 / n, 2.0 / n)
    return weight[:, None] * synthesis(n).T


def derivative_analysis(n):
    derivative = np.zeros((n, n))
    k = np.arange(1, n // 2)
    derivative[k, n // 2 + k] = k
    derivative[n // 2 + k, k] = -k
    return -ALPHA_X * (derivative @ analysis(n))


def waves(n):
    mode = np.arange(n)
    return np.where(mode <= n // 2, mode, mode - n // 2).astype(np.float32)


def halves(table):
    table = np.asarray(table, np.float32)
    top = table.astype(BF16)
    rest = (table - top.astype(np.float32)).astype(BF16)
    return np.concatenate([top, rest], axis=0)


def mode_slots(tail_first):
    slots = -np.ones((NR, 16), np.int64)
    for r in range(NR):
        for k in range(16):
            if tail_first:
                if k >= 8:
                    slots[r, k] = ML * r + k - 8
                elif k >= 4:
                    slots[r, k] = ML * r + 8 + k - 4
            elif k < ML:
                slots[r, k] = ML * r + k
    return slots.reshape(-1)


def tables():
    low_first = np.arange(NZ).reshape(HI, LO).T.reshape(-1)
    sx, sz = synthesis(NX), synthesis(NZ)
    gx, az = derivative_analysis(NX), analysis(NZ)
    forward, backward = [], []
    for tail_first in (False, True):
        slots = mode_slots(tail_first)
        live = slots >= 0
        w = np.zeros((NX, NR * 16))
        w[:, live] = sx[:, slots[live]]
        forward.append(halves(w))
        g = np.zeros((NR * 16, NX))
        g[live] = gx[slots[live]][:, low_first]
        backward.append(halves(g))
    base_x = np.concatenate([sx[:, low::LO] for low in range(LO)], axis=0)
    top, rest = np.split(halves(base_x), 2)
    base_x3 = np.concatenate([top, rest, top], axis=1)
    base_z = np.zeros((NZ, NC, LO, NV))
    base_z[:, :, :, : NZ // NC] = sz.reshape(NZ, NC, 1, NZ // NC)
    return (
        np.stack(forward),
        np.stack(backward),
        halves(sz[:, low_first]),
        halves(az[low_first]),
        base_x3,
        halves(base_z.reshape(NZ, NC * LANES)),
    )


def split2(x):
    top = x.astype(BF16)
    return top, (x - top.astype(F32)).astype(BF16)


def mm(a, b):
    return jnp.dot(a, b, preferred_element_type=F32)


def mm3(table, x):
    rows = table.shape[0] // 2
    top, rest = split2(x)
    both = mm(table, top)
    return both[:rows] + both[rows:] + mm(table[:rows], rest)


def swap_blocks(parts, lane):
    low_half = lane < 64
    even = (lane // NV) % 2 == 0
    v0, v1, v2, v3 = parts

    def pair(x, y, mask, by):
        return (
            jnp.where(mask, x, pltpu.roll(y, by, 1)),
            jnp.where(mask, pltpu.roll(x, LANES - by, 1), y),
        )

    a0, a2 = pair(v0, v2, low_half, 64)
    a1, a3 = pair(v1, v3, low_half, 64)
    b0, b1 = pair(a0, a1, even, 32)
    b2, b3 = pair(a2, a3, even, 32)
    return b0, b1, b2, b3


def step_kernel(
    q_hbm, base_hbm, mask_ref, wz2_ref, decay_ref, to_ref, from_ref,
    fwd_ref, bwd_ref, sz_ref, az_ref, bx_ref, bz_ref,
    stepped_hbm, inverse_ref, growth_ref,
    q_v, send, recv, mid, speed, land, base_v, base_send, base_recv,
    gram_own, gram_col, gram_row_own, gram_row,
    q_sems, base_sem, out_sems,
    fs, fr, bs, br, rs, rr, cs, cr, ws, wr,
):
    r = lax.axis_index("row")
    c = lax.axis_index("col")
    me = r * NC + c
    my_slot = c * NR + r

    for m in range(ML):
        pltpu.make_async_copy(q_hbm.at[m], q_v.at[m], q_sems.at[m]).start()
    base_copy = pltpu.make_async_copy(base_hbm, base_v, base_sem)
    base_copy.start()

    def partner(k):
        off = lax.rem(k * HOP, ND)
        return lax.rem(r + off // NC, NR), lax.rem(c + lax.rem(off, NC), NC)

    barrier = pltpu.get_barrier_semaphore()

    def greet(k, carry):
        r2, c2 = partner(k)
        pl.semaphore_signal(barrier, inc=1, device_id=(r2, c2), device_id_type=MESH)
        return carry

    lax.fori_loop(1, ND, greet, 0)

    base_copy.wait()
    for high in range(BASE):
        for t in range(NY // 8):
            rows = base_v[high * LO, 8 * t : 8 * t + 8, :]
            for low in range(1, LO):
                rows += pltpu.roll(base_v[high * LO + low, 8 * t : 8 * t + 8, :], NV * low, 1)
            base_send[pl.ds(8 * t * BASE + high, 8, stride=BASE), :] = rows

    def pack(m, carry):
        pltpu.make_async_copy(q_hbm.at[m], q_v.at[m], q_sems.at[m]).wait()
        tail = jnp.where(m < 8, 16 + m, 4 + m)
        for j in range(NH // 2):
            for e, at in ((0, m), (1, tail)):
                tile = 2 * j + e
                for t in range(NY // 8):
                    send[pl.ds(8 * t * PIECE + 24 * j + at, 8, stride=PIECE), :] = q_v[
                        m, 8 * t : 8 * t + 8, tile * LANES : (tile + 1) * LANES
                    ]
        return carry

    lax.fori_loop(0, ML, pack, 0)
    pl.semaphore_wait(barrier, ND - 1)

    def send_base(k, carry):
        r2, c2 = partner(k)
        pltpu.make_async_remote_copy(
            base_send.at[pl.ds((r2 * NC + c2) * BASE, BASE)],
            base_recv.at[pl.ds(my_slot * BASE, BASE)],
            bs, br, device_id=(r2, c2), device_id_type=MESH,
        ).start()
        return carry

    lax.fori_loop(1, ND, send_base, 0)

    def send_piece(k, carry):
        r2, c2 = partner(k)
        pltpu.make_async_remote_copy(
            send.at[pl.ds((r2 * NC + c2) * PIECE, PIECE)],
            recv.at[pl.ds(my_slot * PIECE, PIECE)],
            fs, fr, device_id=(r2, c2), device_id_type=MESH,
        ).start()
        return carry

    lax.fori_loop(1, ND, send_piece, 0)

    base_recv[pl.ds(my_slot * BASE, BASE), :] = base_send[pl.ds(me * BASE, BASE), :]
    recv[pl.ds(my_slot * PIECE, PIECE), :] = send[pl.ds(me * PIECE, PIECE), :]

    def drain(ref, rows, sem):
        part = ref.at[pl.ds(0, (ND - 1) * rows)]
        pltpu.make_async_copy(part, part, sem).wait()

    drain(base_recv, BASE, br)
    lane192 = lax.broadcasted_iota(jnp.int32, (NX, 2 * LANES), 1)
    block = (lane192 // NV) % LO
    speed_t = jnp.zeros((NZ, NX), F32)
    for pair in range(NC // 2):
        field = jnp.concatenate(
            [base_recv[(2 * pair + h) * HI : (2 * pair + h + 1) * HI, :] for h in range(2)], axis=1
        )
        top, rest = split2(field)
        out = mm(bx_ref[...], jnp.concatenate([top, top, rest], axis=0))
        half = jnp.zeros((NX, 2 * LANES), F32)
        for low in range(LO):
            half = jnp.where(block == low, out[low * NX : (low + 1) * NX], half)
        top, rest = split2(half)
        table = bz_ref[:, pair * 2 * LANES : (pair + 1) * 2 * LANES]
        nt = (((1,), (1,)), ((), ()))
        both = lax.dot_general(table, top, nt, preferred_element_type=F32)
        speed_t += both[:NZ] + both[NZ:] + lax.dot_general(
            table[:NZ], rest, nt, preferred_element_type=F32
        )
    speed_parts = jnp.concatenate(split2(speed_t), axis=0)
    point = lax.broadcasted_iota(jnp.int32, (NX, 2 * LANES), 0)

    def spread(i, carry):
        pick = (point == 2 * LO * i + lane192 // NV).astype(F32).astype(BF16)
        both = mm(speed_parts, pick)
        speed[i] = both[:NZ] + both[NZ:]
        return carry

    lax.fori_loop(0, HI // 2, spread, 0)

    drain(recv, PIECE, fr)

    def x_forward(i, carry):
        for e in range(2):
            sides = []
            for h in range(2):
                jj = 2 * i + h
                at = (jj // 3) * (NR * PIECE) + lax.rem(jj, 3) * 24 + 8 * e
                sides.append(
                    jnp.concatenate(
                        [
                            recv[pl.ds(pl.multiple_of(at + PIECE * k, 8), 16), :]
                            for k in range(NR)
                        ],
                        axis=0,
                    )
                )
            out = mm3(fwd_ref[e], jnp.concatenate(sides, axis=1))
            for h in range(2):
                tile = 2 * (2 * i + h) + e
                mid[pl.ds(pl.multiple_of(tile * NX, 8), NX), :] = out[:, h * LANES : (h + 1) * LANES]
        return carry

    lax.fori_loop(0, HI // 4, x_forward, 0)

    lane48 = lax.broadcasted_iota(jnp.int32, (HI, LANES), 1)

    def gathered(ref, first):
        return jnp.concatenate(
            [ref[pl.ds(8 * a * NX + first, 8, stride=NX), :] for a in range(HI // 8)], axis=0
        )

    def z_both(i, carry):
        sides = []
        for h in range(2):
            parts = [gathered(mid, (2 * i + h) * LO + low) for low in range(LO)]
            sides.append(jnp.concatenate(swap_blocks(parts, lane48), axis=0))
        physical = mm3(sz_ref[...], jnp.concatenate(sides, axis=1))
        out = mm3(az_ref[...], physical * speed[i])
        for h in range(2):
            recv[pl.ds(pl.multiple_of((2 * i + h) * NX, 8), NX), :] = out[
                :, h * LANES : (h + 1) * LANES
            ]
        return carry

    lax.fori_loop(0, HI // 2, z_both, 0)

    drain(send, PIECE, fs)

    def x_backward(i, carry):
        outs = []
        for e in range(2):
            sides = []
            for h in range(2):
                tile = 2 * (2 * i + h) + e
                parts = [gathered(recv, low * HI + tile) for low in range(LO)]
                sides.append(jnp.concatenate(swap_blocks(parts, lane48), axis=0))
            outs.append(mm3(bwd_ref[e], jnp.concatenate(sides, axis=1)))
        for h in range(2):
            jj = 2 * i + h
            at = (jj // 3) * PIECE + lax.rem(jj, 3) * 24
            cut = slice(h * LANES, (h + 1) * LANES)
            for k in range(NR):
                first = outs[0][16 * k : 16 * k + 16, cut]
                second = outs[1][16 * k : 16 * k + 16, cut]
                group = jnp.concatenate([first[:8], first[8:] + second[:8], second[8:]], axis=0)
                send[pl.ds(pl.multiple_of(at + k * NC * PIECE, 8), 24), :] = group
        return carry

    lax.fori_loop(0, HI // 4, x_backward, 0)

    def send_back(k, carry):
        r2, c2 = partner(k)
        pltpu.make_async_remote_copy(
            send.at[pl.ds((r2 * NC + c2) * PIECE, PIECE)],
            land.at[pl.ds(me * PIECE, PIECE)],
            rs, rr, device_id=(r2, c2), device_id_type=MESH,
        ).start()
        return carry

    lax.fori_loop(1, ND, send_back, 0)
    land[pl.ds(me * PIECE, PIECE), :] = send[pl.ds(me * PIECE, PIECE), :]
    drain(land, PIECE, rr)

    decay = decay_ref[...]

    def solve(m, carry):
        tail = jnp.where(m < 8, 16 + m, 4 + m)
        mode = r * ML + m
        wave = jnp.where(mode <= NX // 2, mode, mode - NX // 2).astype(F32) * ALPHA_X
        for j in range(NH // 2):
            cut = slice(2 * j * LANES, 2 * (j + 1) * LANES)
            tiles = []
            for at in (m, tail):
                tiles.append(
                    jnp.concatenate(
                        [
                            land[pl.ds(8 * t * PIECE + 24 * j + at, 8, stride=PIECE), :]
                            for t in range(NY // 8)
                        ],
                        axis=0,
                    )
                )
            nonlinear = jnp.concatenate(tiles, axis=1) * mask_ref[m, :, cut]
            right = STEP_COEF * q_v[m, :, cut] + nonlinear
            both = mm(to_ref[...], jnp.concatenate(split2(right), axis=0))
            divisor = (STEP_COEF + VISCOSITY * (wave * wave + wz2_ref[:, cut])) + decay
            eigen = (both[:NY] + both[NY:]) / divisor
            both = mm(from_ref[...], jnp.concatenate(split2(eigen), axis=0))
            q_v[m, :, cut] = both[:NY] + both[NY:]
        pltpu.make_async_copy(q_v.at[m], stepped_hbm.at[m], out_sems.at[m]).start()
        return carry

    lax.fori_loop(0, ML, solve, 0)

    def inner(t, carry):
        at = pl.multiple_of(t * LANES, LANES)
        top, rest = split2(q_v[:, :, pl.ds(at, LANES)].reshape(ML * NY, LANES))
        tn = (((0,), (0,)), ((), ()))
        return carry + lax.dot_general(
            top, jnp.concatenate([top, rest], axis=1), tn, preferred_element_type=F32
        )

    whole = lax.fori_loop(0, NH, inner, jnp.zeros((LANES, 2 * LANES), F32))
    cross = whole[:, LANES:]
    whole = whole[:, :LANES] + cross + cross.T
    own = whole[:NV]
    for low in range(1, LO):
        own += pltpu.roll(whole[NV * low : NV * (low + 1)], LANES - NV * low, 1)
    lane32 = lax.broadcasted_iota(jnp.int32, (NV, LANES), 1)
    own = jnp.where(lane32 < NV, own, 0.0)
    packed = own[:8]
    for k in range(1, NV // 8):
        packed += pltpu.roll(own[8 * k : 8 * k + 8], NV * k, 1)

    gram_own[...] = packed
    gram_col[c] = packed

    def send_col(k, carry):
        pltpu.make_async_remote_copy(
            gram_own, gram_col.at[c], cs, cr,
            device_id=(r, lax.rem(c + k, NC)), device_id_type=MESH,
        ).start()
        return carry

    lax.fori_loop(1, NC, send_col, 0)
    part = gram_col.at[pl.ds(0, NC - 1)]
    pltpu.make_async_copy(part, part, cr).wait()
    total = gram_col[0]
    for k in range(1, NC):
        total += gram_col[k]
    gram_row_own[...] = total
    gram_row[r] = total

    def send_row(k, carry):
        pltpu.make_async_remote_copy(
            gram_row_own, gram_row.at[r], ws, wr,
            device_id=(lax.rem(r + k, NR), c), device_id_type=MESH,
        ).start()
        return carry

    lax.fori_loop(1, NR, send_row, 0)
    part = gram_row.at[pl.ds(0, NR - 1)]
    pltpu.make_async_copy(part, part, wr).wait()
    total = gram_row[0]
    for k in range(1, NR):
        total += gram_row[k]

    gram = jnp.concatenate(
        [total] + [pltpu.roll(total, LANES - NV * k, 1) for k in range(1, NV // 8)], axis=0
    )
    gram = gram / float(NX * NY * NZ)
    row32 = lax.broadcasted_iota(jnp.int32, (NV, LANES), 0)
    work = jnp.where(lane32 < NV, gram, jnp.where(lane32 == row32 + NV, 1.0, 0.0))
    for k in range(NV - 1):
        pivot_row = work[k : k + 1, :]
        factor = work[:, k : k + 1] / work[k : k + 1, k : k + 1]
        work = work - jnp.where(row32 > k, factor, 0.0) * pivot_row
    on_diagonal = jnp.where(lane32 == row32, work, 0.0)
    scale = 1.0 / jnp.sqrt(jnp.sum(on_diagonal, axis=1, keepdims=True))
    inverse = pltpu.roll(jnp.where((lane32 >= NV) & (lane32 < 2 * NV), work, 0.0), LANES - NV, 1) * scale
    inverse_ref[...] = jnp.concatenate(
        [inverse] + [pltpu.roll(inverse, NV * k, 1) for k in range(1, LO)], axis=0
    )
    diagonal = jnp.sum(on_diagonal, axis=0, keepdims=True)
    growth_ref[...] = 0.5 * jnp.log(jnp.where(lane32[:1] < NV, diagonal, 1.0))

    drain(base_send, BASE, bs)
    drain(send, PIECE, rs)
    part = gram_col.at[pl.ds(0, NC - 1)]
    pltpu.make_async_copy(part, part, cs).wait()
    part = gram_row.at[pl.ds(0, NR - 1)]
    pltpu.make_async_copy(part, part, ws).wait()
    for m in range(ML):
        pltpu.make_async_copy(q_v.at[m], stepped_hbm.at[m], out_sems.at[m]).wait()


def turn_kernel(stepped_ref, inverse_ref, out_ref):
    top, rest = split2(inverse_ref[...])
    right = jnp.concatenate([top, rest], axis=0)
    right = jnp.concatenate([right, right], axis=1)
    nt = (((1,), (1,)), ((), ()))
    for t in range(NH):
        cut = slice(t * LANES, (t + 1) * LANES)
        left = jnp.concatenate(split2(stepped_ref[0, :, cut]), axis=1)
        both = lax.dot_general(left, right, nt, preferred_element_type=F32)
        out_ref[0, :, cut] = both[:, :LANES] + both[:, LANES:]


def body(tangents, base_flow, mode_mask, decay_rates, to_eigen, from_eigen):
    zv = tangents.shape[2]
    base_wide = jnp.pad(base_flow, ((0, 0), (0, 0), (0, LANES - base_flow.shape[2])))
    mask_wide = jnp.repeat(mode_mask.astype(F32), NV, axis=1).reshape(ML, 1, zv)
    wz2 = jnp.asarray((BETA_Z * np.repeat(waves(NZ), NV)) ** 2, F32).reshape(NC, zv)
    wz2 = lax.dynamic_slice_in_dim(wz2, lax.axis_index("col"), 1, axis=0)
    decay = decay_rates.reshape(NY, 1)

    def stacked(matrix):
        top = lax.reduce_precision(matrix, exponent_bits=8, mantissa_bits=7)
        rest = lax.reduce_precision(matrix - top, exponent_bits=8, mantissa_bits=7)
        both = jnp.concatenate([top, rest], axis=0).astype(BF16)
        return jnp.concatenate([both, both], axis=1)

    constants = [jnp.asarray(t) for t in tables()]
    vmem = pl.BlockSpec(memory_space=pltpu.VMEM)
    anywhere = pl.BlockSpec(memory_space=pl.ANY)
    rows = ND * PIECE
    dma = pltpu.SemaphoreType.DMA
    stepped, inverse, growth = pl.pallas_call(
        step_kernel,
        out_shape=(
            jax.ShapeDtypeStruct(tangents.shape, F32),
            jax.ShapeDtypeStruct((LANES, LANES), F32),
            jax.ShapeDtypeStruct((1, LANES), F32),
        ),
        in_specs=[anywhere, anywhere] + [vmem] * 11,
        out_specs=(anywhere, vmem, vmem),
        scratch_shapes=[
            pltpu.VMEM(tangents.shape, F32),
            pltpu.VMEM((rows, LANES), F32),
            pltpu.VMEM((rows, LANES), F32),
            pltpu.VMEM((HI * NX, LANES), F32),
            pltpu.VMEM((HI // 2, NZ, 2 * LANES), F32),
            pltpu.VMEM((rows, LANES), F32),
            pltpu.VMEM(base_wide.shape, F32),
            pltpu.VMEM((ND * BASE, LANES), F32),
            pltpu.VMEM((ND * BASE, LANES), F32),
            pltpu.VMEM((8, LANES), F32),
            pltpu.VMEM((NC, 8, LANES), F32),
            pltpu.VMEM((8, LANES), F32),
            pltpu.VMEM((NR, 8, LANES), F32),
            dma((ML,)), dma, dma((ML,)),
        ] + [dma] * 10,
        compiler_params=pltpu.CompilerParams(
            collective_id=0, has_side_effects=True, vmem_limit_bytes=60 * 2**20
        ),
        name="step",
    )(tangents, base_wide, mask_wide, wz2, decay, stacked(to_eigen), stacked(from_eigen), *constants)

    block = pl.BlockSpec((1, NY, zv), lambda m: (m, 0, 0))
    vectors = pl.pallas_call(
        turn_kernel,
        grid=(ML,),
        out_shape=jax.ShapeDtypeStruct(tangents.shape, F32),
        in_specs=[block, pl.BlockSpec((LANES, LANES), lambda m: (0, 0))],
        out_specs=block,
        name="turn",
    )(stepped, inverse)
    return vectors, growth[0, :NV]


def solution(mesh):
    placed = (P("row", None, "col"), P("row", None, "col"), P("row", "col"), P(), P(), P())
    return jax.shard_map(
        body, mesh=mesh, in_specs=placed, out_specs=(P("row", None, "col"), P()), check_vma=False
    )
```

```python
import functools
import math

import jax
import jax.numpy as jnp
import numpy as np
from jax import lax
from jax.experimental import pallas as pl
from jax.experimental.pallas import tpu as pltpu
from jax.sharding import PartitionSpec as P

MESH = pl.DeviceIdType.MESH
F32 = jnp.float32
BF16 = jnp.bfloat16
STEP_COEF = 10.0
VISCOSITY = 0.01
ALPHA_X = 0.5
BETA_Z = 1.0

NX = 192
NY = 128
NZ = 192
NV = 32
NR, NC = 16, 8
ND = NR * NC
ML = NX // NR
LANES = 128
LO = LANES // NV
HI = NZ // LO
NH = HI // NC
PIECE = ML * NH
BASE = ML // LO
CHUNKS = NH // 2
PART = PIECE // CHUNKS
SPAN = ND * PART
HOP = 37


def synthesis(n):
    point = np.arange(n)[:, None]
    mode = np.arange(n)[None, :]
    wave = np.where(mode <= n // 2, mode, mode - n // 2)
    angle = (point * wave % n) * (2.0 * math.pi / n)
    return np.where(mode <= n // 2, np.cos(angle), np.sin(angle))


def analysis(n):
    mode = np.arange(n)
    weight = np.where((mode == 0) | (mode == n // 2), 1.0 / n, 2.0 / n)
    return weight[:, None] * synthesis(n).T


def derivative_analysis(n):
    derivative = np.zeros((n, n))
    k = np.arange(1, n // 2)
    derivative[k, n // 2 + k] = k
    derivative[n // 2 + k, k] = -k
    return -ALPHA_X * (derivative @ analysis(n))


def waves(n):
    mode = np.arange(n)
    return np.where(mode <= n // 2, mode, mode - n // 2).astype(np.float32)


def halves(table):
    table = np.asarray(table, np.float32)
    top = table.astype(BF16)
    rest = (table - top.astype(np.float32)).astype(BF16)
    return np.concatenate([top, rest], axis=0)


def mode_slots(tail_first):
    slots = -np.ones((NR, 16), np.int64)
    for r in range(NR):
        for k in range(16):
            if tail_first:
                if k >= 8:
                    slots[r, k] = ML * r + k - 8
                elif k >= 4:
                    slots[r, k] = ML * r + 8 + k - 4
            elif k < ML:
                slots[r, k] = ML * r + k
    return slots.reshape(-1)


def tables():
    low_first = np.arange(NZ).reshape(HI, LO).T.reshape(-1)
    sx, sz = synthesis(NX), synthesis(NZ)
    gx, az = derivative_analysis(NX), analysis(NZ)
    forward, backward = [], []
    for tail_first in (False, True):
        slots = mode_slots(tail_first)
        live = slots >= 0
        w = np.zeros((NX, NR * 16))
        w[:, live] = sx[:, slots[live]]
        forward.append(halves(w))
        g = np.zeros((NR * 16, NX))
        g[live] = gx[slots[live]][:, low_first]
        backward.append(halves(g))
    base_x = np.concatenate([sx[:, low::LO] for low in range(LO)], axis=0)
    top, rest = np.split(halves(base_x), 2)
    base_x3 = np.concatenate([top, rest, top], axis=1)
    base_z = np.zeros((NZ, NC, LO, NV))
    base_z[:, :, :, : NZ // NC] = sz.reshape(NZ, NC, 1, NZ // NC)
    return (
        np.stack(forward),
        np.stack(backward),
        halves(sz[:, low_first]),
        halves(az[low_first]),
        base_x3,
        halves(base_z.reshape(NZ, NC * LANES)),
    )


def split2(x):
    top = x.astype(BF16)
    return top, (x - top.astype(F32)).astype(BF16)


def mm(a, b):
    return jnp.dot(a, b, preferred_element_type=F32)


def mm3(table, x):
    rows = table.shape[0] // 2
    top, rest = split2(x)
    both = mm(table, top)
    return both[:rows] + both[rows:] + mm(table[:rows], rest)


def swap_blocks(parts, lane):
    low_half = lane < 64
    even = (lane // NV) % 2 == 0
    v0, v1, v2, v3 = parts

    def pair(x, y, mask, by):
        return (
            jnp.where(mask, x, pltpu.roll(y, by, 1)),
            jnp.where(mask, pltpu.roll(x, LANES - by, 1), y),
        )

    a0, a2 = pair(v0, v2, low_half, 64)
    a1, a3 = pair(v1, v3, low_half, 64)
    b0, b1 = pair(a0, a1, even, 32)
    b2, b3 = pair(a2, a3, even, 32)
    return b0, b1, b2, b3


def step_kernel(
    q_hbm, base_hbm, mask_hbm, decay_hbm, to_hbm, from_hbm,
    fwd_hbm, bwd_hbm, sz_hbm, az_hbm, bx_hbm, bz_hbm,
    stepped_hbm, inverse_ref, growth_ref,
    q_v, send, recv, mid, speed, land,
    base_v, base_send, base_recv, mask_v, mask_w, decay_v, to_v, from_v, to_s, from_s,
    fwd_v, bwd_v, sz_v, az_v, bx_v, bz_v,
    gram_own, gram_col, gram_row_own, gram_row,
    q_sems, in_sems, out_sems, fr, rr,
    fs, bs, br, rs, cs, cr, ws, wr,
):
    r = lax.axis_index("row")
    c = lax.axis_index("col")
    me = r * NC + c
    my_slot = c * NR + r
    wide = 2 * LANES

    def cut(j):
        return slice(wide * j, wide * (j + 1))

    small = [
        pltpu.make_async_copy(src, dst, in_sems.at[k])
        for k, (src, dst) in enumerate(
            [
                (base_hbm, base_v), (bx_hbm, bx_v), (bz_hbm, bz_v), (fwd_hbm, fwd_v),
                (sz_hbm, sz_v), (az_hbm, az_v), (bwd_hbm, bwd_v), (mask_hbm, mask_v),
                (decay_hbm, decay_v), (to_hbm, to_v), (from_hbm, from_v),
            ]
        )
    ]
    loads = [
        pltpu.make_async_copy(q_hbm.at[:, :, cut(j)], q_v.at[:, :, cut(j)], q_sems.at[j])
        for j in range(CHUNKS)
    ]
    small[0].start()
    for copy in loads:
        copy.start()
    for copy in small[1:]:
        copy.start()

    def partner(k):
        off = lax.rem(k * HOP, ND)
        return lax.rem(r + off // NC, NR), lax.rem(c + lax.rem(off, NC), NC)

    barrier = pltpu.get_barrier_semaphore()

    def greet(k, carry):
        r2, c2 = partner(k)
        pl.semaphore_signal(barrier, inc=1, device_id=(r2, c2), device_id_type=MESH)
        return carry

    lax.fori_loop(1, ND, greet, 0)

    small[0].wait()
    gap = jnp.zeros((NV - NZ // NC, NY), F32)
    for high in range(BASE):
        stack = []
        for low in range(LO):
            stack += [base_v[high * LO + low], gap]
        turned = jnp.concatenate(stack, axis=0).T
        for t in range(NY // 8):
            base_send[pl.ds(8 * t * BASE + high, 8, stride=BASE), :] = turned[8 * t : 8 * t + 8]

    def tail_row(m):
        return jnp.where(m < 8, 16 + m, 4 + m)

    def pack(j):
        loads[j].wait()

        def one(m, carry):
            for e, at in ((0, m), (1, tail_row(m))):
                tile = slice((2 * j + e) * LANES, (2 * j + e + 1) * LANES)
                for t in range(NY // 8):
                    send[pl.ds(j * SPAN + 8 * t * PART + at, 8, stride=PART), :] = q_v[
                        m, 8 * t : 8 * t + 8, tile
                    ]
            return carry

        lax.fori_loop(0, ML, one, 0, unroll=2)

    def send_forward(j):
        def one(k, carry):
            r2, c2 = partner(k)
            pltpu.make_async_remote_copy(
                send.at[pl.ds(j * SPAN + (r2 * NC + c2) * PART, PART)],
                recv.at[pl.ds(j * SPAN + my_slot * PART, PART)],
                fs, fr.at[j], device_id=(r2, c2), device_id_type=MESH,
            ).start()
            return carry

        lax.fori_loop(1, ND, one, 0)

    def send_base(k, carry):
        r2, c2 = partner(k)
        pltpu.make_async_remote_copy(
            base_send.at[pl.ds((r2 * NC + c2) * BASE, BASE)],
            base_recv.at[pl.ds(my_slot * BASE, BASE)],
            bs, br, device_id=(r2, c2), device_id_type=MESH,
        ).start()
        return carry

    pack(0)
    pl.semaphore_wait(barrier, ND - 1)
    lax.fori_loop(1, ND, send_base, 0)
    send_forward(0)
    for j in range(1, CHUNKS):
        pack(j)
        send_forward(j)

    base_recv[pl.ds(my_slot * BASE, BASE), :] = base_send[pl.ds(me * BASE, BASE), :]
    for j in range(CHUNKS):
        recv[pl.ds(j * SPAN + my_slot * PART, PART), :] = send[pl.ds(j * SPAN + me * PART, PART), :]

    def drain(ref, first, rows, sem):
        part = ref.at[pl.ds(first, (ND - 1) * rows)]
        pltpu.make_async_copy(part, part, sem).wait()

    for copy in small[1:]:
        copy.wait()
    for src, dst in ((to_v, to_s), (from_v, from_s)):
        both = jnp.concatenate(split2(src[...]), axis=0)
        dst[...] = jnp.concatenate([both, both], axis=1)
    zv = NZ // NC * NV
    column = lax.broadcasted_iota(jnp.int32, (NZ // NC, zv), 1) // NV
    pick = (lax.broadcasted_iota(jnp.int32, (NZ // NC, zv), 0) == column).astype(F32)
    mask_w[...] = mm(mask_v[...].astype(F32).astype(BF16), pick.astype(BF16))

    drain(base_recv, 0, BASE, br)
    lane192 = lax.broadcasted_iota(jnp.int32, (NX, wide), 1)
    block = (lane192 // NV) % LO
    speed_t = jnp.zeros((NZ, NX), F32)
    nt = (((1,), (1,)), ((), ()))
    for pair in range(NC // 2):
        field = jnp.concatenate(
            [base_recv[(2 * pair + h) * HI : (2 * pair + h + 1) * HI, :] for h in range(2)], axis=1
        )
        top, rest = split2(field)
        out = mm(bx_v[...], jnp.concatenate([top, top, rest], axis=0))
        half = jnp.zeros((NX, wide), F32)
        for low in range(LO):
            half = jnp.where(block == low, out[low * NX : (low + 1) * NX], half)
        top, rest = split2(half)
        table = bz_v[:, cut(pair)]
        both = lax.dot_general(table, top, nt, preferred_element_type=F32)
        speed_t += both[:NZ] + both[NZ:] + lax.dot_general(
            table[:NZ], rest, nt, preferred_element_type=F32
        )
    speed_parts = jnp.concatenate(split2(speed_t), axis=0)
    point = lax.broadcasted_iota(jnp.int32, (NX, wide), 0)

    def spread(i, carry):
        pick = (point == 2 * LO * i + lane192 // NV).astype(F32).astype(BF16)
        both = mm(speed_parts, pick)
        speed[i] = both[:NZ] + both[NZ:]
        return carry

    lax.fori_loop(0, HI // 2, spread, 0)

    def x_forward(j):
        def one(i, carry):
            for e in range(2):
                sides = []
                for h in range(2):
                    at = j * SPAN + (2 * i + h) * (NR * PART) + 8 * e
                    sides.append(
                        jnp.concatenate(
                            [
                                recv[pl.ds(pl.multiple_of(at + PART * k, 8), 16), :]
                                for k in range(NR)
                            ],
                            axis=0,
                        )
                    )
                out = mm3(fwd_v[e], jnp.concatenate(sides, axis=1))
                for h in range(2):
                    tile = NH * (2 * i + h) + 2 * j + e
                    mid[pl.ds(pl.multiple_of(tile * NX, 8), NX), :] = out[
                        :, h * LANES : (h + 1) * LANES
                    ]
            return carry

        lax.fori_loop(0, NC // 2, one, 0, unroll=2)

    for j in range(CHUNKS):
        drain(recv, j * SPAN, PART, fr.at[j])
        x_forward(j)

    lane48 = lax.broadcasted_iota(jnp.int32, (HI, LANES), 1)

    def gathered(ref, first):
        return jnp.concatenate(
            [ref[pl.ds(8 * a * NX + first, 8, stride=NX), :] for a in range(HI // 8)], axis=0
        )

    def z_both(i, carry):
        sides = []
        for h in range(2):
            parts = [gathered(mid, (2 * i + h) * LO + low) for low in range(LO)]
            sides.append(jnp.concatenate(swap_blocks(parts, lane48), axis=0))
        physical = mm3(sz_v[...], jnp.concatenate(sides, axis=1))
        out = mm3(az_v[...], physical * speed[i])
        for h in range(2):
            recv[pl.ds(pl.multiple_of((2 * i + h) * NX, 8), NX), :] = out[
                :, h * LANES : (h + 1) * LANES
            ]
        return carry

    lax.fori_loop(0, HI // 2, z_both, 0, unroll=4)

    def x_backward(j):
        def one(i, carry):
            outs = []
            for e in range(2):
                sides = []
                for h in range(2):
                    tile = NH * (2 * i + h) + 2 * j + e
                    parts = [gathered(recv, low * HI + tile) for low in range(LO)]
                    sides.append(jnp.concatenate(swap_blocks(parts, lane48), axis=0))
                outs.append(mm3(bwd_v[e], jnp.concatenate(sides, axis=1)))
            for h in range(2):
                side = slice(h * LANES, (h + 1) * LANES)
                for k in range(NR):
                    first = outs[0][16 * k : 16 * k + 16, side]
                    second = outs[1][16 * k : 16 * k + 16, side]
                    group = jnp.concatenate(
                        [first[:8], first[8:] + second[:8], second[8:]], axis=0
                    )
                    at = j * SPAN + (k * NC + 2 * i + h) * PART
                    send[pl.ds(pl.multiple_of(at, 8), PART), :] = group
            return carry

        lax.fori_loop(0, NC // 2, one, 0, unroll=2)

    def send_back(j):
        def one(k, carry):
            r2, c2 = partner(k)
            pltpu.make_async_remote_copy(
                send.at[pl.ds(j * SPAN + (r2 * NC + c2) * PART, PART)],
                land.at[pl.ds(j * SPAN + me * PART, PART)],
                rs, rr.at[j], device_id=(r2, c2), device_id_type=MESH,
            ).start()
            return carry

        lax.fori_loop(1, ND, one, 0)

    drain(send, 0, PIECE, fs)
    for j in range(CHUNKS):
        x_backward(j)
        send_back(j)
        land[pl.ds(j * SPAN + me * PART, PART), :] = send[pl.ds(j * SPAN + me * PART, PART), :]

    decay = jnp.broadcast_to(decay_v[...], (NY, NY)).T
    decay = jnp.concatenate([decay, decay], axis=1)

    def wave_of(mode, count):
        return jnp.where(mode <= count // 2, mode, mode - count // 2).astype(F32)

    def solve(j):
        lane = lax.broadcasted_iota(jnp.int32, (1, wide), 1)
        wave_z = BETA_Z * wave_of(c * (NZ // NC) + 2 * LO * j + lane // NV, NZ)
        square_z = wave_z * wave_z

        def one(m, carry):
            wave_x = ALPHA_X * wave_of(r * ML + m, NX)
            tiles = []
            for at in (m, tail_row(m)):
                tiles.append(
                    jnp.concatenate(
                        [
                            land[pl.ds(j * SPAN + 8 * t * PART + at, 8, stride=PART), :]
                            for t in range(NY // 8)
                        ],
                        axis=0,
                    )
                )
            nonlinear = jnp.concatenate(tiles, axis=1) * mask_w[pl.ds(m, 1), cut(j)]
            right = STEP_COEF * q_v[m, :, cut(j)] + nonlinear
            both = mm(to_s[...], jnp.concatenate(split2(right), axis=0))
            divisor = (STEP_COEF + VISCOSITY * (wave_x * wave_x + square_z)) + decay
            eigen = (both[:NY] + both[NY:]) / divisor
            both = mm(from_s[...], jnp.concatenate(split2(eigen), axis=0))
            q_v[m, :, cut(j)] = both[:NY] + both[NY:]
            return carry

        lax.fori_loop(0, ML, one, 0, unroll=3)

    def inner(tile):
        at = slice(tile * LANES, (tile + 1) * LANES)
        top, rest = split2(q_v[:, :, at].reshape(ML * NY, LANES))
        tn = (((0,), (0,)), ((), ()))
        return lax.dot_general(
            top, jnp.concatenate([top, rest], axis=1), tn, preferred_element_type=F32
        )

    stores = [
        pltpu.make_async_copy(q_v.at[:, :, cut(j)], stepped_hbm.at[:, :, cut(j)], out_sems.at[j])
        for j in range(CHUNKS)
    ]
    whole = jnp.zeros((LANES, wide), F32)
    for j in range(CHUNKS):
        drain(land, j * SPAN, PART, rr.at[j])
        solve(j)
        stores[j].start()
        whole += inner(2 * j) + inner(2 * j + 1)

    cross = whole[:, LANES:]
    whole = whole[:, :LANES] + cross + cross.T
    own = whole[:NV]
    for low in range(1, LO):
        own += pltpu.roll(whole[NV * low : NV * (low + 1)], LANES - NV * low, 1)
    lane32 = lax.broadcasted_iota(jnp.int32, (NV, LANES), 1)
    own = jnp.where(lane32 < NV, own, 0.0)
    packed = own[:8]
    for k in range(1, NV // 8):
        packed += pltpu.roll(own[8 * k : 8 * k + 8], NV * k, 1)

    gram_own[...] = packed
    gram_col[c] = packed

    def send_col(k, carry):
        pltpu.make_async_remote_copy(
            gram_own, gram_col.at[c], cs, cr,
            device_id=(r, lax.rem(c + k, NC)), device_id_type=MESH,
        ).start()
        return carry

    lax.fori_loop(1, NC, send_col, 0)
    part = gram_col.at[pl.ds(0, NC - 1)]
    pltpu.make_async_copy(part, part, cr).wait()
    total = gram_col[0]
    for k in range(1, NC):
        total += gram_col[k]
    gram_row_own[...] = total
    gram_row[r] = total

    def send_row(k, carry):
        pltpu.make_async_remote_copy(
            gram_row_own, gram_row.at[r], ws, wr,
            device_id=(lax.rem(r + k, NR), c), device_id_type=MESH,
        ).start()
        return carry

    lax.fori_loop(1, NR, send_row, 0)
    part = gram_row.at[pl.ds(0, NR - 1)]
    pltpu.make_async_copy(part, part, wr).wait()
    total = gram_row[0]
    for k in range(1, NR):
        total += gram_row[k]

    gram = jnp.concatenate(
        [total] + [pltpu.roll(total, LANES - NV * k, 1) for k in range(1, NV // 8)], axis=0
    )
    gram = gram / float(NX * NY * NZ)
    row32 = lax.broadcasted_iota(jnp.int32, (NV, LANES), 0)
    work = jnp.where(lane32 < NV, gram, jnp.where(lane32 == row32 + NV, 1.0, 0.0))
    for k in range(NV - 1):
        pivot_row = work[k : k + 1, :]
        factor = work[:, k : k + 1] / work[k : k + 1, k : k + 1]
        work = work - jnp.where(row32 > k, factor, 0.0) * pivot_row
    on_diagonal = jnp.where(lane32 == row32, work, 0.0)
    scale = 1.0 / jnp.sqrt(jnp.sum(on_diagonal, axis=1, keepdims=True))
    keep = (lane32 >= NV) & (lane32 < 2 * NV)
    inverse = pltpu.roll(jnp.where(keep, work, 0.0), LANES - NV, 1) * scale
    inverse_ref[...] = jnp.concatenate(
        [inverse] + [pltpu.roll(inverse, NV * k, 1) for k in range(1, LO)], axis=0
    )
    diagonal = jnp.sum(on_diagonal, axis=0, keepdims=True)
    growth_ref[...] = 0.5 * jnp.log(jnp.where(lane32[:1] < NV, diagonal, 1.0))

    drain(base_send, 0, BASE, bs)
    drain(send, 0, PIECE, rs)
    part = gram_col.at[pl.ds(0, NC - 1)]
    pltpu.make_async_copy(part, part, cs).wait()
    part = gram_row.at[pl.ds(0, NR - 1)]
    pltpu.make_async_copy(part, part, ws).wait()
    for copy in stores:
        copy.wait()


def turn_kernel(stepped_ref, inverse_ref, growth_ref, out_ref, growth_out):
    top, rest = split2(inverse_ref[...])
    right = jnp.concatenate([top, rest], axis=0)
    right = jnp.concatenate([right, right], axis=1)
    nt = (((1,), (1,)), ((), ()))
    rows = stepped_ref[...].reshape(ML * NY, LANES)
    both = lax.dot_general(
        jnp.concatenate(split2(rows), axis=1), right, nt, preferred_element_type=F32
    )
    out_ref[...] = (both[:, :LANES] + both[:, LANES:]).reshape(ML, NY, LANES)
    growth_out[...] = growth_ref[:, :NV]


def body(tangents, base_flow, mode_mask, decay_rates, to_eigen, from_eigen):
    constants = [jnp.asarray(t) for t in tables()]
    inputs = [
        tangents, jnp.transpose(base_flow, (0, 2, 1)), mode_mask, decay_rates.reshape(1, NY),
        to_eigen, from_eigen,
    ] + constants
    vmem = pl.BlockSpec(memory_space=pltpu.VMEM)
    anywhere = pl.BlockSpec(memory_space=pl.ANY)
    dma = pltpu.SemaphoreType.DMA
    field = pltpu.VMEM((ND * PIECE, LANES), F32)
    stepped, inverse, growth = pl.pallas_call(
        step_kernel,
        out_shape=(
            jax.ShapeDtypeStruct(tangents.shape, F32),
            jax.ShapeDtypeStruct((LANES, LANES), F32),
            jax.ShapeDtypeStruct((1, LANES), F32),
        ),
        in_specs=[anywhere] * len(inputs),
        out_specs=(anywhere, vmem, vmem),
        scratch_shapes=[
            pltpu.VMEM(tangents.shape, F32), field, field, field,
            pltpu.VMEM((HI // 2, NZ, 2 * LANES), F32), field,
            pltpu.VMEM(inputs[1].shape, F32),
            pltpu.VMEM((ND * BASE, LANES), F32),
            pltpu.VMEM((ND * BASE, LANES), F32),
            pltpu.VMEM(mode_mask.shape, jnp.int32),
            pltpu.VMEM((ML, tangents.shape[2]), F32),
            pltpu.VMEM((1, NY), F32),
            pltpu.VMEM((NY, NY), F32),
            pltpu.VMEM((NY, NY), F32),
            pltpu.VMEM((2 * NY, 2 * NY), BF16),
            pltpu.VMEM((2 * NY, 2 * NY), BF16),
        ]
        + [pltpu.VMEM(t.shape, t.dtype) for t in constants]
        + [
            pltpu.VMEM((8, LANES), F32),
            pltpu.VMEM((NC, 8, LANES), F32),
            pltpu.VMEM((8, LANES), F32),
            pltpu.VMEM((NR, 8, LANES), F32),
            dma((CHUNKS,)), dma((len(inputs) - 1,)), dma((CHUNKS,)), dma((CHUNKS,)), dma((CHUNKS,)),
        ]
        + [dma] * 8,
        compiler_params=pltpu.CompilerParams(
            collective_id=0, has_side_effects=True, vmem_limit_bytes=60 * 2**20
        ),
        name="step",
    )(*inputs)

    block = pl.BlockSpec((ML, NY, LANES), lambda t: (0, 0, t))
    vectors, growth = pl.pallas_call(
        turn_kernel,
        grid=(NH,),
        out_shape=(
            jax.ShapeDtypeStruct(tangents.shape, F32),
            jax.ShapeDtypeStruct((1, NV), F32),
        ),
        in_specs=[
            block,
            pl.BlockSpec((LANES, LANES), lambda t: (0, 0)),
            pl.BlockSpec((1, LANES), lambda t: (0, 0)),
        ],
        out_specs=(block, pl.BlockSpec((1, NV), lambda t: (0, 0))),
        name="turn",
    )(stepped, inverse, growth)
    return vectors, growth.reshape(NV)


def solution(mesh):
    placed = (P("row", None, "col"), P("row", None, "col"), P("row", "col"), P(), P(), P())
    return jax.shard_map(
        body, mesh=mesh, in_specs=placed, out_specs=(P("row", None, "col"), P()), check_vma=False
    )
```

```python
import functools
import math

import jax
import jax.numpy as jnp
import numpy as np
from jax import lax
from jax.experimental import pallas as pl
from jax.experimental.pallas import tpu as pltpu
from jax.sharding import PartitionSpec as P

MESH = pl.DeviceIdType.MESH
F32 = jnp.float32
BF16 = jnp.bfloat16
STEP_COEF = 10.0
VISCOSITY = 0.01
ALPHA_X = 0.5
BETA_Z = 1.0

NX = 192
NY = 128
NZ = 192
NV = 32
NR, NC = 16, 8
ND = NR * NC
ML = NX // NR
NL = NZ // NC
LANES = 128
HALVES = 2
VH = NV // HALVES
LO = LANES // VH
HI = NZ // LO
TILES = HI // NC
PIECE = ML * TILES
PITCH = 40
SPAN = ND * PITCH
EARLY = 24
BLO = LANES // NV
BHI = NX // BLO
BASE = ML // BLO
QUAD = 4
HOP = 37


def synthesis(n):
    point = np.arange(n)[:, None]
    mode = np.arange(n)[None, :]
    wave = np.where(mode <= n // 2, mode, mode - n // 2)
    angle = (point * wave % n) * (2.0 * math.pi / n)
    return np.where(mode <= n // 2, np.cos(angle), np.sin(angle))


def analysis(n):
    mode = np.arange(n)
    weight = np.where((mode == 0) | (mode == n // 2), 1.0 / n, 2.0 / n)
    return weight[:, None] * synthesis(n).T


def derivative_analysis(n):
    derivative = np.zeros((n, n))
    k = np.arange(1, n // 2)
    derivative[k, n // 2 + k] = k
    derivative[n // 2 + k, k] = -k
    return -ALPHA_X * (derivative @ analysis(n))


def waves(n):
    mode = np.arange(n)
    return np.where(mode <= n // 2, mode, mode - n // 2).astype(np.float32)


def halves(table):
    table = np.asarray(table, np.float32)
    top = table.astype(BF16)
    rest = (table - top.astype(np.float32)).astype(BF16)
    return np.concatenate([top, rest], axis=0)


def mode_slots(tail_first):
    slots = -np.ones((NR, 16), np.int64)
    for r in range(NR):
        for k in range(16):
            if tail_first:
                if k >= 8:
                    slots[r, k] = ML * r + k - 8
                elif k >= 4:
                    slots[r, k] = ML * r + 8 + k - 4
            elif k < ML:
                slots[r, k] = ML * r + k
    return slots.reshape(-1)


def spanwise_of(block):
    return block // 2 + 4 * (block % 2)


def tables():
    low, high = np.arange(LO)[:, None], np.arange(HI)[None, :]
    modes = (LO * high + spanwise_of(low)).reshape(-1)
    points = (LO * high + low).reshape(-1)
    sx, sz = synthesis(NX), synthesis(NZ)
    gx, az = derivative_analysis(NX), analysis(NZ)
    forward, backward = [], []
    for tail_first in (False, True):
        slots = mode_slots(tail_first)
        live = slots >= 0
        w = np.zeros((NX, NR * 16))
        w[:, live] = sx[:, slots[live]]
        forward.append(halves(w))
        g = np.zeros((NR * 16, NX))
        g[live] = gx[slots[live]][:, points]
        backward.append(halves(g))
    base_x = np.concatenate([sx[:, k::BLO] for k in range(BLO)], axis=0)
    top, rest = np.split(halves(base_x), 2)
    base_x3 = np.concatenate([top, rest, top], axis=1)
    base_z = np.zeros((NZ, NC, BLO, NV))
    base_z[:, :, :, :NL] = sz.reshape(NZ, NC, 1, NL)
    return (
        np.stack(forward),
        np.stack(backward),
        halves(sz[:, modes]),
        halves(az[modes]),
        base_x3,
        halves(base_z.reshape(NZ, NC * LANES)),
    )


def split2(x):
    top = x.astype(BF16)
    return top, (x - top.astype(F32)).astype(BF16)


def mm(a, b):
    return jnp.dot(a, b, preferred_element_type=F32)


def mm3(table, x):
    rows = table.shape[0] // 2
    top, rest = split2(x)
    both = mm(table, top)
    return both[:rows] + both[rows:] + mm(table[:rows], rest)


def even_blocks(lane, width):
    return (lane // width) % 2 == 0


def pair_up(x, y, lane, width):
    mask = even_blocks(lane, width)
    return (
        jnp.where(mask, x, pltpu.roll(y, width, 1)),
        jnp.where(mask, pltpu.roll(x, LANES - width, 1), y),
    )


def swap_blocks(parts, lane):
    parts = list(parts)
    bit = LO // 2
    while bit:
        for k in range(LO):
            if not k & bit:
                parts[k], parts[k | bit] = pair_up(parts[k], parts[k | bit], lane, VH * bit)
        bit //= 2
    return parts


def step_kernel(
    q_hbm, base_hbm, mask_hbm, decay_hbm, to_hbm, from_hbm,
    fwd_hbm, bwd_hbm, sz_hbm, az_hbm, bx_hbm, bz_hbm,
    stepped_hbm, inverse_ref, growth_ref,
    q_v, send, recv, mid, speed, land,
    base_v, base_send, base_recv, mask_v, mask_w, decay_v, to_v, from_v, to_s, from_s,
    fwd_v, bwd_v, sz_v, az_v, bx_v, bz_v,
    gram_own, gram_col, gram_row_own, gram_row,
    q_sems, in_sems, out_sems, fs, fr, rr,
    bs, br, rs, cs, cr, ws, wr,
):
    r = lax.axis_index("row")
    c = lax.axis_index("col")
    me = r * NC + c
    my_slot = c * NR + r
    wide = 2 * LANES

    def cut(j):
        return slice(wide * j, wide * (j + 1))

    def tile(t):
        return slice(LANES * t, LANES * (t + 1))

    small = [
        pltpu.make_async_copy(src, dst, in_sems.at[k])
        for k, (src, dst) in enumerate(
            [
                (base_hbm, base_v), (bx_hbm, bx_v), (bz_hbm, bz_v), (fwd_hbm, fwd_v),
                (sz_hbm, sz_v), (az_hbm, az_v), (bwd_hbm, bwd_v), (mask_hbm, mask_v),
                (decay_hbm, decay_v), (to_hbm, to_v), (from_hbm, from_v),
            ]
        )
    ]
    loads = [
        pltpu.make_async_copy(q_hbm.at[:, :, cut(j)], q_v.at[:, :, cut(j)], q_sems.at[j])
        for j in range(TILES)
    ]
    small[0].start()
    for copy in loads:
        copy.start()
    for copy in small[1:]:
        copy.start()

    def partner(k):
        off = lax.rem(k * HOP, ND)
        return lax.rem(r + off // NC, NR), lax.rem(c + lax.rem(off, NC), NC)

    barrier = pltpu.get_barrier_semaphore()

    def greet(k, carry):
        r2, c2 = partner(k)
        pl.semaphore_signal(barrier, inc=1, device_id=(r2, c2), device_id_type=MESH)
        return carry

    lax.fori_loop(1, ND, greet, 0)

    def clear(k, carry):
        recv[pl.ds(PITCH * k + PIECE, PITCH - PIECE), :] = jnp.zeros((PITCH - PIECE, LANES), F32)
        return carry

    lax.fori_loop(0, HALVES * ND, clear, 0)

    small[0].wait()
    gap = jnp.zeros((NV - NL, NY), F32)
    for high in range(BASE):
        stack = []
        for low in range(BLO):
            stack += [base_v[high * BLO + low], gap]
        turned = jnp.concatenate(stack, axis=0).T
        for t in range(NY // 8):
            base_send[pl.ds(8 * t * BASE + high, 8, stride=BASE), :] = turned[8 * t : 8 * t + 8]

    def row_of(j, m):
        return (m, jnp.where(m < 8, 16 + m, 4 + m), 24 + m)[j]

    def half_of(first, second, lane, h):
        return pair_up(first, second, lane, VH)[h]

    lane8 = lax.broadcasted_iota(jnp.int32, (8, LANES), 1)

    def pack(h):
        def one(m, carry):
            for j in range(TILES):
                for t in range(NY // 8):
                    rows = slice(8 * t, 8 * t + 8)
                    send[pl.ds(h * SPAN + 8 * t * PITCH + row_of(j, m), 8, stride=PITCH), :] = half_of(
                        q_v[m, rows, tile(2 * j)], q_v[m, rows, tile(2 * j + 1)], lane8, h
                    )
            return carry

        lax.fori_loop(0, ML, one, 0)

    def send_forward(h):
        def one(k, carry):
            r2, c2 = partner(k)
            pltpu.make_async_remote_copy(
                send.at[pl.ds(h * SPAN + (r2 * NC + c2) * PITCH, PIECE)],
                recv.at[pl.ds(h * SPAN + my_slot * PITCH, PIECE)],
                fs.at[h], fr.at[h], device_id=(r2, c2), device_id_type=MESH,
            ).start()
            return carry

        lax.fori_loop(1, ND, one, 0)

    def send_base(k, carry):
        r2, c2 = partner(k)
        pltpu.make_async_remote_copy(
            base_send.at[pl.ds((r2 * NC + c2) * BASE, BASE)],
            base_recv.at[pl.ds(my_slot * BASE, BASE)],
            bs, br, device_id=(r2, c2), device_id_type=MESH,
        ).start()
        return carry

    def keep_own(dst, to, h):
        dst[pl.ds(pl.multiple_of(h * SPAN + to * PITCH, 8), PIECE), :] = send[
            pl.ds(pl.multiple_of(h * SPAN + me * PITCH, 8), PIECE), :
        ]

    for copy in loads:
        copy.wait()
    pack(0)
    pl.semaphore_wait(barrier, ND - 1)
    lax.fori_loop(1, ND, send_base, 0)
    send_forward(0)
    pack(1)
    send_forward(1)
    base_recv[pl.ds(my_slot * BASE, BASE), :] = base_send[pl.ds(me * BASE, BASE), :]
    for h in range(HALVES):
        keep_own(recv, my_slot, h)

    def drain(ref, first, rows, sem):
        part = ref.at[pl.ds(first, (ND - 1) * rows)]
        pltpu.make_async_copy(part, part, sem).wait()

    for copy in small[1:]:
        copy.wait()
    for src, dst in ((to_v, to_s), (from_v, from_s)):
        both = jnp.concatenate(split2(src[...]), axis=0)
        dst[...] = jnp.concatenate([both, both], axis=1)
    spot = lax.broadcasted_iota(jnp.int32, (NL, TILES * LANES), 1) // VH
    column = LO * (spot // LO) + spanwise_of(lax.rem(spot, LO))
    pick = lax.broadcasted_iota(jnp.int32, (NL, TILES * LANES), 0) == column
    retained = mm(mask_v[...].astype(F32).astype(BF16), pick.astype(F32).astype(BF16))
    for j in range(TILES):
        mask_w[16 * j : 16 * j + ML, :] = retained[:, tile(j)]

    drain(base_recv, 0, BASE, br)
    block = (lax.broadcasted_iota(jnp.int32, (NX, wide), 1) // NV) % BLO
    speed_t = jnp.zeros((NZ, NX), F32)
    nt = (((1,), (1,)), ((), ()))
    for pair in range(NC // 2):
        field = jnp.concatenate(
            [base_recv[(2 * pair + h) * BHI : (2 * pair + h + 1) * BHI, :] for h in range(2)],
            axis=1,
        )
        top, rest = split2(field)
        out = mm(bx_v[...], jnp.concatenate([top, top, rest], axis=0))
        half = jnp.zeros((NX, wide), F32)
        for low in range(BLO):
            half = jnp.where(block == low, out[low * NX : (low + 1) * NX], half)
        top, rest = split2(half)
        table = bz_v[:, cut(pair)]
        both = lax.dot_general(table, top, nt, preferred_element_type=F32)
        speed_t += both[:NZ] + both[NZ:] + lax.dot_general(
            table[:NZ], rest, nt, preferred_element_type=F32
        )
    speed_parts = jnp.concatenate(split2(speed_t), axis=0)
    spread_shape = (NX, QUAD * LANES)
    point = lax.broadcasted_iota(jnp.int32, spread_shape, 0)
    spot_x = lax.broadcasted_iota(jnp.int32, spread_shape, 1) // VH

    def spread(i, carry):
        pick = (point == QUAD * LO * i + spot_x).astype(F32).astype(BF16)
        both = mm(speed_parts, pick)
        speed[i] = both[:NZ] + both[NZ:]
        return carry

    lax.fori_loop(0, HI // QUAD, spread, 0)

    types = ((0, (0, 2)), (1, (1,)))
    first_row = (0, 8, 24)

    def x_forward(h):
        def one(i, carry):
            for e, tiles in types:
                at = [(2 * i + k, j) for k in range(2) for j in tiles]
                sides = []
                for c2, j in at:
                    base = h * SPAN + c2 * (NR * PITCH) + first_row[j]
                    sides.append(
                        jnp.concatenate(
                            [
                                recv[pl.ds(pl.multiple_of(base + PITCH * k, 8), 16), :]
                                for k in range(NR)
                            ],
                            axis=0,
                        )
                    )
                out = mm3(fwd_v[e], jnp.concatenate(sides, axis=1))
                for k, (c2, j) in enumerate(at):
                    to = (TILES * c2 + j) * NX
                    mid[pl.ds(pl.multiple_of(to, 8), NX), :] = out[:, tile(k)]
            return carry

        lax.fori_loop(0, NC // 2, one, 0, unroll=2)

    lane24 = lax.broadcasted_iota(jnp.int32, (HI, LANES), 1)

    def gathered(ref, first):
        return jnp.concatenate(
            [ref[pl.ds(8 * a * NX + first, 8, stride=NX), :] for a in range(HI // 8)], axis=0
        )

    def swapped(ref, starts):
        parts = [gathered(ref, first) for first in starts]
        return jnp.concatenate(swap_blocks(parts, lane24), axis=0)

    def z_both(h):
        def one(i, carry):
            sides = [
                swapped(mid, [(QUAD * i + k) * LO + low for low in range(LO)]) for k in range(QUAD)
            ]
            physical = mm3(sz_v[...], jnp.concatenate(sides, axis=1))
            out = mm3(az_v[...], physical * speed[i])
            for k in range(QUAD):
                to = h * SPAN + (QUAD * i + k) * NX
                recv[pl.ds(pl.multiple_of(to, 8), NX), :] = out[:, tile(k)]
            return carry

        lax.fori_loop(0, HI // QUAD, one, 0, unroll=3)

    def x_backward(h):
        def one(i, carry):
            done = {}
            for e, tiles in types:
                at = [(k, j) for k in range(2) for j in tiles]
                sides = []
                for k, j in at:
                    high = TILES * (2 * i + k) + j
                    sides.append(swapped(recv, [h * SPAN + low * HI + high for low in range(LO)]))
                out = mm3(bwd_v[e], jnp.concatenate(sides, axis=1))
                for k, key in enumerate(at):
                    done[key] = out[:, tile(k)]
            for k in range(2):
                for r2 in range(NR):
                    t0, t1, t2 = (done[k, j][16 * r2 : 16 * r2 + 16] for j in range(TILES))
                    to = h * SPAN + (r2 * NC + 2 * i + k) * PITCH
                    send[pl.ds(pl.multiple_of(to, 8), PITCH), :] = jnp.concatenate(
                        [t0[:8], t0[8:] + t1[:8], t1[8:], t2], axis=0
                    )
            return carry

        lax.fori_loop(0, NC // 2, one, 0, unroll=2)

    def send_back(h, first, rows, sem):
        def one(k, carry):
            r2, c2 = partner(k)
            pltpu.make_async_remote_copy(
                send.at[pl.ds(h * SPAN + (r2 * NC + c2) * PITCH + first, rows)],
                land.at[pl.ds(h * SPAN + me * PITCH + first, rows)],
                rs, sem, device_id=(r2, c2), device_id_type=MESH,
            ).start()
            return carry

        lax.fori_loop(1, ND, one, 0)

    for h in range(HALVES):
        drain(recv, h * SPAN, PIECE, fr.at[h])
        x_forward(h)
        z_both(h)
        drain(send, h * SPAN, PIECE, fs.at[h])
        x_backward(h)
        if h < HALVES - 1:
            send_back(h, 0, PIECE, rr.at[0])
        else:
            send_back(h, 0, EARLY, rr.at[1])
            send_back(h, EARLY, PIECE - EARLY, rr.at[2])
        keep_own(land, me, h)

    decay = jnp.broadcast_to(decay_v[...], (NY, NY)).T
    decay = jnp.concatenate([decay, decay], axis=1)
    lane128 = lax.broadcasted_iota(jnp.int32, (NY, LANES), 1)
    spot = lax.broadcasted_iota(jnp.int32, (1, LANES), 1) // VH

    def wave_of(mode, count):
        return jnp.where(mode <= count // 2, mode, mode - count // 2).astype(F32)

    def solve(h, j):
        wave_z = BETA_Z * wave_of(c * NL + LO * j + spanwise_of(spot), NZ)
        square_z = wave_z * wave_z

        def one(i, carry):
            right, squares = [], []
            for m in (2 * i, 2 * i + 1):
                nonlinear = jnp.concatenate(
                    [
                        land[pl.ds(h * SPAN + 8 * t * PITCH + row_of(j, m), 8, stride=PITCH), :]
                        for t in range(NY // 8)
                    ],
                    axis=0,
                )
                field = half_of(q_v[m, :, tile(2 * j)], q_v[m, :, tile(2 * j + 1)], lane128, h)
                right.append(STEP_COEF * field + nonlinear * mask_w[pl.ds(16 * j + m, 1), :])
                wave_x = ALPHA_X * wave_of(r * ML + m, NX)
                squares.append(wave_x * wave_x + square_z)
            right = jnp.concatenate(right, axis=1)
            both = mm(to_s[...], jnp.concatenate(split2(right), axis=0))
            divisor = (STEP_COEF + VISCOSITY * jnp.concatenate(squares, axis=1)) + decay
            eigen = (both[:NY] + both[NY:]) / divisor
            both = mm(from_s[...], jnp.concatenate(split2(eigen), axis=0))
            stepped = both[:NY] + both[NY:]
            for k, m in enumerate((2 * i, 2 * i + 1)):
                kept = pl.ds(pl.multiple_of((j * ML + m) * NY, 8), NY)
                if h < HALVES - 1:
                    mid[kept, :] = stepped[:, tile(k)]
                else:
                    first, second = pair_up(mid[kept, :], stepped[:, tile(k)], lane128, VH)
                    q_v[m, :, tile(2 * j)] = first
                    q_v[m, :, tile(2 * j + 1)] = second
            return carry

        lax.fori_loop(0, ML // 2, one, 0, unroll=3)

    def inner(t):
        top, rest = split2(q_v[:, :, tile(t)].reshape(ML * NY, LANES))
        tn = (((0,), (0,)), ((), ()))
        return lax.dot_general(
            top, jnp.concatenate([top, rest], axis=1), tn, preferred_element_type=F32
        )

    stores = [
        pltpu.make_async_copy(q_v.at[:, :, cut(j)], stepped_hbm.at[:, :, cut(j)], out_sems.at[j])
        for j in range(TILES)
    ]
    drain(land, 0, PIECE, rr.at[0])
    for j in range(TILES):
        solve(0, j)
    whole = jnp.zeros((LANES, wide), F32)
    for j in range(TILES):
        if j == 0:
            drain(land, SPAN, EARLY, rr.at[1])
        if j == TILES - 1:
            drain(land, SPAN, PIECE - EARLY, rr.at[2])
        solve(1, j)
        stores[j].start()
        whole += inner(2 * j) + inner(2 * j + 1)

    cross = whole[:, LANES:]
    whole = whole[:, :LANES] + cross + cross.T
    own = whole[:NV]
    for low in range(1, BLO):
        own += pltpu.roll(whole[NV * low : NV * (low + 1)], LANES - NV * low, 1)
    lane32 = lax.broadcasted_iota(jnp.int32, (NV, LANES), 1)
    own = jnp.where(lane32 < NV, own, 0.0)
    packed = own[:8]
    for k in range(1, NV // 8):
        packed += pltpu.roll(own[8 * k : 8 * k + 8], NV * k, 1)

    gram_own[...] = packed
    gram_col[c] = packed

    def send_col(k, carry):
        pltpu.make_async_remote_copy(
            gram_own, gram_col.at[c], cs, cr,
            device_id=(r, lax.rem(c + k, NC)), device_id_type=MESH,
        ).start()
        return carry

    lax.fori_loop(1, NC, send_col, 0)
    part = gram_col.at[pl.ds(0, NC - 1)]
    pltpu.make_async_copy(part, part, cr).wait()
    total = gram_col[0]
    for k in range(1, NC):
        total += gram_col[k]
    gram_row_own[...] = total
    gram_row[r] = total

    def send_row(k, carry):
        pltpu.make_async_remote_copy(
            gram_row_own, gram_row.at[r], ws, wr,
            device_id=(lax.rem(r + k, NR), c), device_id_type=MESH,
        ).start()
        return carry

    lax.fori_loop(1, NR, send_row, 0)
    part = gram_row.at[pl.ds(0, NR - 1)]
    pltpu.make_async_copy(part, part, wr).wait()
    total = gram_row[0]
    for k in range(1, NR):
        total += gram_row[k]

    gram = jnp.concatenate(
        [total] + [pltpu.roll(total, LANES - NV * k, 1) for k in range(1, NV // 8)], axis=0
    )
    gram = gram / float(NX * NY * NZ)
    row32 = lax.broadcasted_iota(jnp.int32, (NV, LANES), 0)
    work = jnp.where(lane32 < NV, gram, jnp.where(lane32 == row32 + NV, 1.0, 0.0))
    for k in range(NV - 1):
        pivot_row = work[k : k + 1, :]
        factor = work[:, k : k + 1] / work[k : k + 1, k : k + 1]
        work = work - jnp.where(row32 > k, factor, 0.0) * pivot_row
    on_diagonal = jnp.where(lane32 == row32, work, 0.0)
    scale = 1.0 / jnp.sqrt(jnp.sum(on_diagonal, axis=1, keepdims=True))
    keep = (lane32 >= NV) & (lane32 < 2 * NV)
    inverse = pltpu.roll(jnp.where(keep, work, 0.0), LANES - NV, 1) * scale
    inverse_ref[...] = jnp.concatenate(
        [inverse] + [pltpu.roll(inverse, NV * k, 1) for k in range(1, BLO)], axis=0
    )
    diagonal = jnp.sum(on_diagonal, axis=0, keepdims=True)
    growth_ref[...] = 0.5 * jnp.log(jnp.where(lane32[:1] < NV, diagonal, 1.0))

    drain(base_send, 0, BASE, bs)
    drain(send, 0, HALVES * PIECE, rs)
    part = gram_col.at[pl.ds(0, NC - 1)]
    pltpu.make_async_copy(part, part, cs).wait()
    part = gram_row.at[pl.ds(0, NR - 1)]
    pltpu.make_async_copy(part, part, ws).wait()
    for copy in stores:
        copy.wait()


def turn_kernel(stepped_hbm, inverse_ref, growth_ref, out_hbm, growth_out, x_v, y_v, in_sems, out_sems):
    def load(t):
        at = pl.ds(pl.multiple_of(t * LANES, LANES), LANES)
        return pltpu.make_async_copy(stepped_hbm.at[:, :, at], x_v.at[t], in_sems.at[t])

    def store(t):
        at = pl.ds(pl.multiple_of(t * LANES, LANES), LANES)
        return pltpu.make_async_copy(y_v.at[t], out_hbm.at[:, :, at], out_sems.at[t])

    count = x_v.shape[0]
    for t in range(count):
        load(t).start()
    top, rest = split2(inverse_ref[...])
    right = jnp.concatenate([top, rest], axis=0)
    right = jnp.concatenate([right, right], axis=1)
    growth_out[...] = growth_ref[:, :NV]

    def one(t, carry):
        load(t).wait()
        nt = (((1,), (1,)), ((), ()))
        rows = x_v[t].reshape(ML * NY, LANES)
        both = lax.dot_general(
            jnp.concatenate(split2(rows), axis=1), right, nt, preferred_element_type=F32
        )
        y_v[t] = (both[:, :LANES] + both[:, LANES:]).reshape(ML, NY, LANES)
        store(t).start()
        return carry

    lax.fori_loop(0, count, one, 0)
    for t in range(count):
        store(t).wait()


def body(tangents, base_flow, mode_mask, decay_rates, to_eigen, from_eigen):
    constants = [jnp.asarray(t) for t in tables()]
    inputs = [
        tangents, jnp.transpose(base_flow, (0, 2, 1)), mode_mask, decay_rates.reshape(1, NY),
        to_eigen, from_eigen,
    ] + constants
    vmem = pl.BlockSpec(memory_space=pltpu.VMEM)
    anywhere = pl.BlockSpec(memory_space=pl.ANY)
    dma = pltpu.SemaphoreType.DMA
    field = pltpu.VMEM((HALVES * SPAN, LANES), F32)
    stepped, inverse, growth = pl.pallas_call(
        step_kernel,
        out_shape=(
            jax.ShapeDtypeStruct(tangents.shape, F32),
            jax.ShapeDtypeStruct((LANES, LANES), F32),
            jax.ShapeDtypeStruct((1, LANES), F32),
        ),
        in_specs=[anywhere] * len(inputs),
        out_specs=(anywhere, vmem, vmem),
        scratch_shapes=[
            pltpu.VMEM(tangents.shape, F32), field, field,
            pltpu.VMEM((HI * NX, LANES), F32),
            pltpu.VMEM((HI // QUAD, NZ, QUAD * LANES), F32), field,
            pltpu.VMEM(inputs[1].shape, F32),
            pltpu.VMEM((ND * BASE, LANES), F32),
            pltpu.VMEM((ND * BASE, LANES), F32),
            pltpu.VMEM(mode_mask.shape, jnp.int32),
            pltpu.VMEM((16 * TILES, LANES), F32),
            pltpu.VMEM((1, NY), F32),
            pltpu.VMEM((NY, NY), F32),
            pltpu.VMEM((NY, NY), F32),
            pltpu.VMEM((2 * NY, 2 * NY), BF16),
            pltpu.VMEM((2 * NY, 2 * NY), BF16),
        ]
        + [pltpu.VMEM(t.shape, t.dtype) for t in constants]
        + [
            pltpu.VMEM((8, LANES), F32),
            pltpu.VMEM((NC, 8, LANES), F32),
            pltpu.VMEM((8, LANES), F32),
            pltpu.VMEM((NR, 8, LANES), F32),
            dma((TILES,)), dma((len(inputs) - 1,)), dma((TILES,)),
            dma((HALVES,)), dma((HALVES,)), dma((3,)),
        ]
        + [dma] * 7,
        compiler_params=pltpu.CompilerParams(
            collective_id=0, has_side_effects=True, vmem_limit_bytes=60 * 2**20
        ),
        name="step",
    )(*inputs)

    tiles = tangents.shape[2] // LANES
    vectors, growth = pl.pallas_call(
        turn_kernel,
        out_shape=(
            jax.ShapeDtypeStruct(tangents.shape, F32),
            jax.ShapeDtypeStruct((1, NV), F32),
        ),
        in_specs=[anywhere, vmem, vmem],
        out_specs=(anywhere, vmem),
        scratch_shapes=[
            pltpu.VMEM((tiles, ML, NY, LANES), F32),
            pltpu.VMEM((tiles, ML, NY, LANES), F32),
            dma((tiles,)), dma((tiles,)),
        ],
        compiler_params=pltpu.CompilerParams(vmem_limit_bytes=40 * 2**20),
        name="turn",
    )(stepped, inverse, growth)
    return vectors, growth.reshape(NV)


def solution(mesh):
    placed = (P("row", None, "col"), P("row", None, "col"), P("row", "col"), P(), P(), P())
    return jax.shard_map(
        body, mesh=mesh, in_specs=placed, out_specs=(P("row", None, "col"), P()), check_vma=False
    )
```

```python
import functools
import math

import jax
import jax.numpy as jnp
import numpy as np
from jax import lax
from jax.experimental import pallas as pl
from jax.experimental.pallas import tpu as pltpu
from jax.sharding import PartitionSpec as P

MESH = pl.DeviceIdType.MESH
F32 = jnp.float32
BF16 = jnp.bfloat16
STEP_COEF = 10.0
VISCOSITY = 0.01
ALPHA_X = 0.5
BETA_Z = 1.0

NX = 192
NY = 128
NZ = 192
NV = 32
NR, NC = 16, 8
ND = NR * NC
ML = NX // NR
NL = NZ // NC
LANES = 128
HALVES = 2
VH = NV // HALVES
LO = LANES // VH
HI = NZ // LO
TILES = HI // NC
PIECE = ML * TILES
PITCH = 40
SPAN = ND * PITCH
EARLY = 24
BLO = LANES // NV
BHI = NX // BLO
BASE = ML // BLO
QUAD = 4
HOP = 101


def synthesis(n):
    point = np.arange(n)[:, None]
    mode = np.arange(n)[None, :]
    wave = np.where(mode <= n // 2, mode, mode - n // 2)
    angle = (point * wave % n) * (2.0 * math.pi / n)
    return np.where(mode <= n // 2, np.cos(angle), np.sin(angle))


def analysis(n):
    mode = np.arange(n)
    weight = np.where((mode == 0) | (mode == n // 2), 1.0 / n, 2.0 / n)
    return weight[:, None] * synthesis(n).T


def derivative_analysis(n):
    derivative = np.zeros((n, n))
    k = np.arange(1, n // 2)
    derivative[k, n // 2 + k] = k
    derivative[n // 2 + k, k] = -k
    return -ALPHA_X * (derivative @ analysis(n))


def waves(n):
    mode = np.arange(n)
    return np.where(mode <= n // 2, mode, mode - n // 2).astype(np.float32)


def halves(table):
    table = np.asarray(table, np.float32)
    top = table.astype(BF16)
    rest = (table - top.astype(np.float32)).astype(BF16)
    return np.concatenate([top, rest], axis=0)


def mode_slots(tail_first):
    slots = -np.ones((NR, 16), np.int64)
    for r in range(NR):
        for k in range(16):
            if tail_first:
                if k >= 8:
                    slots[r, k] = ML * r + k - 8
                elif k >= 4:
                    slots[r, k] = ML * r + 8 + k - 4
            elif k < ML:
                slots[r, k] = ML * r + k
    return slots.reshape(-1)


def spanwise_of(block):
    return block // 2 + 4 * (block % 2)


def tables():
    low, high = np.arange(LO)[:, None], np.arange(HI)[None, :]
    modes = (LO * high + spanwise_of(low)).reshape(-1)
    points = (LO * high + low).reshape(-1)
    sx, sz = synthesis(NX), synthesis(NZ)
    gx, az = derivative_analysis(NX), analysis(NZ)
    forward, backward = [], []
    for tail_first in (False, True):
        slots = mode_slots(tail_first)
        live = slots >= 0
        w = np.zeros((NX, NR * 16))
        w[:, live] = sx[:, slots[live]]
        forward.append(halves(w))
        g = np.zeros((NR * 16, NX))
        g[live] = gx[slots[live]][:, points]
        backward.append(halves(g))
    base_x = np.concatenate([sx[:, k::BLO] for k in range(BLO)], axis=0)
    top, rest = np.split(halves(base_x), 2)
    base_x3 = np.concatenate([top, rest, top], axis=1)
    base_z = np.zeros((NZ, NC, BLO, NV))
    base_z[:, :, :, :NL] = sz.reshape(NZ, NC, 1, NL)
    return (
        np.stack(forward),
        np.stack(backward),
        halves(sz[:, modes]),
        halves(az[modes]),
        base_x3,
        halves(base_z.reshape(NZ, NC * LANES)),
    )


def split2(x):
    top = x.astype(BF16)
    return top, (x - top.astype(F32)).astype(BF16)


def mm(a, b):
    return jnp.dot(a, b, preferred_element_type=F32)


def mm3(table, x):
    rows = table.shape[0] // 2
    top, rest = split2(x)
    both = mm(table, top)
    return both[:rows] + both[rows:] + mm(table[:rows], rest)


def even_blocks(lane, width):
    return (lane // width) % 2 == 0


def pair_up(x, y, lane, width):
    mask = even_blocks(lane, width)
    return (
        jnp.where(mask, x, pltpu.roll(y, width, 1)),
        jnp.where(mask, pltpu.roll(x, LANES - width, 1), y),
    )


def swap_blocks(parts, lane):
    parts = list(parts)
    bit = LO // 2
    while bit:
        for k in range(LO):
            if not k & bit:
                parts[k], parts[k | bit] = pair_up(parts[k], parts[k | bit], lane, VH * bit)
        bit //= 2
    return parts


def farthest_first(side):
    offsets = [
        (y, x, z, core)
        for y in range(side) for x in range(side) for z in range(side) for core in range(2)
    ]
    hops = lambda offset: sum(min(k, side - k) for k in offset[:3])
    return sorted(offsets[1:], key=hops, reverse=True)


def step_kernel(
    q_hbm, base_hbm, mask_hbm, decay_hbm, to_hbm, from_hbm,
    fwd_hbm, bwd_hbm, sz_hbm, az_hbm, bx_hbm, bz_hbm,
    stepped_hbm, gram_ref,
    q_v, send, recv, mid, speed, land,
    base_v, base_send, base_recv, mask_v, mask_w, decay_v, to_v, from_v, to_s, from_s,
    fwd_v, bwd_v, sz_v, az_v, bx_v, bz_v,
    gram_own, gram_col, gram_row_own, gram_row,
    q_sems, in_sems, out_sems, fs, fr, rr,
    bs, br, rs, cs, cr, ws, wr,
):
    r = lax.axis_index("row")
    c = lax.axis_index("col")
    me = r * NC + c
    my_slot = c * NR + r
    wide = 2 * LANES

    def cut(j):
        return slice(wide * j, wide * (j + 1))

    def tile(t):
        return slice(LANES * t, LANES * (t + 1))

    small = [
        pltpu.make_async_copy(src, dst, in_sems.at[k])
        for k, (src, dst) in enumerate(
            [
                (base_hbm, base_v), (bx_hbm, bx_v), (bz_hbm, bz_v), (fwd_hbm, fwd_v),
                (sz_hbm, sz_v), (az_hbm, az_v), (bwd_hbm, bwd_v), (mask_hbm, mask_v),
                (decay_hbm, decay_v), (to_hbm, to_v), (from_hbm, from_v),
            ]
        )
    ]
    loads = [
        pltpu.make_async_copy(q_hbm.at[:, :, cut(j)], q_v.at[:, :, cut(j)], q_sems.at[j])
        for j in range(TILES)
    ]
    small[0].start()
    for copy in loads:
        copy.start()
    for copy in small[1:]:
        copy.start()

    def partner(k):
        off = lax.rem(k * HOP, ND)
        return lax.rem(r + off // NC, NR), lax.rem(c + lax.rem(off, NC), NC)

    barrier = pltpu.get_barrier_semaphore()

    side = 4
    ys = [lax.rem(r // side + k, side) * side for k in range(side)]
    xs = [lax.rem(lax.rem(r, side) + k, side) for k in range(side)]
    zs = [lax.rem(c // 2 + k, side) * 2 for k in range(side)]
    cores = [lax.rem(c, 2), 1 - lax.rem(c, 2)]
    for y, x, z, core in farthest_first(side):
        pl.semaphore_signal(
            barrier, inc=1, device_id=(ys[y] + xs[x], zs[z] + cores[core]), device_id_type=MESH
        )

    small[0].wait()
    gap = jnp.zeros((NV - NL, NY), F32)
    for high in range(BASE):
        stack = []
        for low in range(BLO):
            stack += [base_v[high * BLO + low], gap]
        turned = jnp.concatenate(stack, axis=0).T
        for t in range(NY // 8):
            base_send[pl.ds(8 * t * BASE + high, 8, stride=BASE), :] = turned[8 * t : 8 * t + 8]

    def row_of(j, m):
        return (m, jnp.where(m < 8, 16 + m, 4 + m), 24 + m)[j]

    def half_of(first, second, lane, h):
        return pair_up(first, second, lane, VH)[h]

    lane8 = lax.broadcasted_iota(jnp.int32, (8, LANES), 1)

    def pack(h):
        def one(m, carry):
            for j in range(TILES):
                for t in range(NY // 8):
                    rows = slice(8 * t, 8 * t + 8)
                    send[pl.ds(h * SPAN + 8 * t * PITCH + row_of(j, m), 8, stride=PITCH), :] = half_of(
                        q_v[m, rows, tile(2 * j)], q_v[m, rows, tile(2 * j + 1)], lane8, h
                    )
            return carry

        lax.fori_loop(0, ML, one, 0)

    def send_forward(h):
        def one(k, carry):
            r2, c2 = partner(k)
            pltpu.make_async_remote_copy(
                send.at[pl.ds(h * SPAN + (r2 * NC + c2) * PITCH, PIECE)],
                recv.at[pl.ds(h * SPAN + my_slot * PITCH, PIECE)],
                fs.at[h], fr.at[h], device_id=(r2, c2), device_id_type=MESH,
            ).start()
            return carry

        lax.fori_loop(1, ND, one, 0)

    def send_base(k, carry):
        r2, c2 = partner(k)
        pltpu.make_async_remote_copy(
            base_send.at[pl.ds((r2 * NC + c2) * BASE, BASE)],
            base_recv.at[pl.ds(my_slot * BASE, BASE)],
            bs, br, device_id=(r2, c2), device_id_type=MESH,
        ).start()
        return carry

    def keep_own(dst, to, h):
        dst[pl.ds(pl.multiple_of(h * SPAN + to * PITCH, 8), PIECE), :] = send[
            pl.ds(pl.multiple_of(h * SPAN + me * PITCH, 8), PIECE), :
        ]

    for copy in loads:
        copy.wait()
    pack(0)

    def clear(k, carry):
        recv[pl.ds(PITCH * k + PIECE, PITCH - PIECE), :] = jnp.zeros((PITCH - PIECE, LANES), F32)
        return carry

    lax.fori_loop(0, HALVES * ND, clear, 0, unroll=4)
    pl.semaphore_wait(barrier, ND - 1)
    lax.fori_loop(1, ND, send_base, 0)
    send_forward(0)
    pack(1)
    send_forward(1)
    base_recv[pl.ds(my_slot * BASE, BASE), :] = base_send[pl.ds(me * BASE, BASE), :]
    for h in range(HALVES):
        keep_own(recv, my_slot, h)

    def drain(ref, first, rows, sem):
        part = ref.at[pl.ds(first, (ND - 1) * rows)]
        pltpu.make_async_copy(part, part, sem).wait()

    for copy in small[1:]:
        copy.wait()
    for src, dst in ((to_v, to_s), (from_v, from_s)):
        both = jnp.concatenate(split2(src[...]), axis=0)
        dst[...] = jnp.concatenate([both, both], axis=1)
    spot = lax.broadcasted_iota(jnp.int32, (NL, TILES * LANES), 1) // VH
    column = LO * (spot // LO) + spanwise_of(lax.rem(spot, LO))
    pick = lax.broadcasted_iota(jnp.int32, (NL, TILES * LANES), 0) == column
    retained = mm(mask_v[...].astype(F32).astype(BF16), pick.astype(F32).astype(BF16))
    for j in range(TILES):
        mask_w[16 * j : 16 * j + ML, :] = retained[:, tile(j)]

    drain(base_recv, 0, BASE, br)
    block = (lax.broadcasted_iota(jnp.int32, (NX, wide), 1) // NV) % BLO
    speed_t = jnp.zeros((NZ, NX), F32)
    nt = (((1,), (1,)), ((), ()))
    for pair in range(NC // 2):
        field = jnp.concatenate(
            [base_recv[(2 * pair + h) * BHI : (2 * pair + h + 1) * BHI, :] for h in range(2)],
            axis=1,
        )
        top, rest = split2(field)
        out = mm(bx_v[...], jnp.concatenate([top, top, rest], axis=0))
        half = jnp.zeros((NX, wide), F32)
        for low in range(BLO):
            half = jnp.where(block == low, out[low * NX : (low + 1) * NX], half)
        top, rest = split2(half)
        table = bz_v[:, cut(pair)]
        both = lax.dot_general(table, top, nt, preferred_element_type=F32)
        speed_t += both[:NZ] + both[NZ:] + lax.dot_general(
            table[:NZ], rest, nt, preferred_element_type=F32
        )
    speed_parts = jnp.concatenate(split2(speed_t), axis=0)
    spread_shape = (NX, QUAD * LANES)
    point = lax.broadcasted_iota(jnp.int32, spread_shape, 0)
    spot_x = lax.broadcasted_iota(jnp.int32, spread_shape, 1) // VH

    def spread(i, carry):
        pick = (point == QUAD * LO * i + spot_x).astype(F32).astype(BF16)
        both = mm(speed_parts, pick)
        speed[i] = both[:NZ] + both[NZ:]
        return carry

    lax.fori_loop(0, HI // QUAD, spread, 0)

    types = ((0, (0, 2)), (1, (1,)))
    first_row = (0, 8, 24)

    def x_forward(h):
        def one(i, carry):
            for e, tiles in types:
                at = [(2 * i + k, j) for k in range(2) for j in tiles]
                sides = []
                for c2, j in at:
                    base = h * SPAN + c2 * (NR * PITCH) + first_row[j]
                    sides.append(
                        jnp.concatenate(
                            [
                                recv[pl.ds(pl.multiple_of(base + PITCH * k, 8), 16), :]
                                for k in range(NR)
                            ],
                            axis=0,
                        )
                    )
                out = mm3(fwd_v[e], jnp.concatenate(sides, axis=1))
                for k, (c2, j) in enumerate(at):
                    to = (TILES * c2 + j) * NX
                    mid[pl.ds(pl.multiple_of(to, 8), NX), :] = out[:, tile(k)]
            return carry

        lax.fori_loop(0, NC // 2, one, 0, unroll=2)

    lane24 = lax.broadcasted_iota(jnp.int32, (HI, LANES), 1)

    def gathered(ref, first):
        return jnp.concatenate(
            [ref[pl.ds(8 * a * NX + first, 8, stride=NX), :] for a in range(HI // 8)], axis=0
        )

    def swapped(ref, starts):
        parts = [gathered(ref, first) for first in starts]
        return jnp.concatenate(swap_blocks(parts, lane24), axis=0)

    def z_both(h):
        def one(i, carry):
            sides = [
                swapped(mid, [(QUAD * i + k) * LO + low for low in range(LO)]) for k in range(QUAD)
            ]
            physical = mm3(sz_v[...], jnp.concatenate(sides, axis=1))
            out = mm3(az_v[...], physical * speed[i])
            for k in range(QUAD):
                to = h * SPAN + (QUAD * i + k) * NX
                recv[pl.ds(pl.multiple_of(to, 8), NX), :] = out[:, tile(k)]
            return carry

        lax.fori_loop(0, HI // QUAD, one, 0, unroll=2)

    def x_backward(h):
        def one(i, carry):
            done = {}
            for e, tiles in types:
                at = [(k, j) for k in range(2) for j in tiles]
                sides = []
                for k, j in at:
                    high = TILES * (2 * i + k) + j
                    sides.append(swapped(recv, [h * SPAN + low * HI + high for low in range(LO)]))
                out = mm3(bwd_v[e], jnp.concatenate(sides, axis=1))
                for k, key in enumerate(at):
                    done[key] = out[:, tile(k)]
            for k in range(2):
                for r2 in range(NR):
                    t0, t1, t2 = (done[k, j][16 * r2 : 16 * r2 + 16] for j in range(TILES))
                    to = h * SPAN + (r2 * NC + 2 * i + k) * PITCH
                    send[pl.ds(pl.multiple_of(to, 8), PITCH), :] = jnp.concatenate(
                        [t0[:8], t0[8:] + t1[:8], t1[8:], t2], axis=0
                    )
            return carry

        lax.fori_loop(0, NC // 2, one, 0)

    def send_back(h, first, rows, sem):
        def one(k, carry):
            r2, c2 = partner(k)
            pltpu.make_async_remote_copy(
                send.at[pl.ds(h * SPAN + (r2 * NC + c2) * PITCH + first, rows)],
                land.at[pl.ds(h * SPAN + me * PITCH + first, rows)],
                rs, sem, device_id=(r2, c2), device_id_type=MESH,
            ).start()
            return carry

        lax.fori_loop(1, ND, one, 0)

    for h in range(HALVES):
        drain(recv, h * SPAN, PIECE, fr.at[h])
        x_forward(h)
        z_both(h)
        drain(send, h * SPAN, PIECE, fs.at[h])
        x_backward(h)
        if h < HALVES - 1:
            send_back(h, 0, PIECE, rr.at[0])
        else:
            send_back(h, 0, EARLY, rr.at[1])
            send_back(h, EARLY, PIECE - EARLY, rr.at[2])
        keep_own(land, me, h)

    decay = jnp.broadcast_to(decay_v[...], (NY, NY)).T
    decay = jnp.concatenate([decay, decay], axis=1)
    lane128 = lax.broadcasted_iota(jnp.int32, (NY, LANES), 1)
    spot = lax.broadcasted_iota(jnp.int32, (1, LANES), 1) // VH

    def wave_of(mode, count):
        return jnp.where(mode <= count // 2, mode, mode - count // 2).astype(F32)

    def solve(h, j):
        wave_z = BETA_Z * wave_of(c * NL + LO * j + spanwise_of(spot), NZ)
        square_z = wave_z * wave_z

        def one(i, carry):
            right, squares = [], []
            for m in (2 * i, 2 * i + 1):
                nonlinear = jnp.concatenate(
                    [
                        land[pl.ds(h * SPAN + 8 * t * PITCH + row_of(j, m), 8, stride=PITCH), :]
                        for t in range(NY // 8)
                    ],
                    axis=0,
                )
                field = half_of(q_v[m, :, tile(2 * j)], q_v[m, :, tile(2 * j + 1)], lane128, h)
                right.append(STEP_COEF * field + nonlinear * mask_w[pl.ds(16 * j + m, 1), :])
                wave_x = ALPHA_X * wave_of(r * ML + m, NX)
                squares.append(wave_x * wave_x + square_z)
            right = jnp.concatenate(right, axis=1)
            both = mm(to_s[...], jnp.concatenate(split2(right), axis=0))
            divisor = (STEP_COEF + VISCOSITY * jnp.concatenate(squares, axis=1)) + decay
            eigen = (both[:NY] + both[NY:]) / divisor
            both = mm(from_s[...], jnp.concatenate(split2(eigen), axis=0))
            stepped = both[:NY] + both[NY:]
            for k, m in enumerate((2 * i, 2 * i + 1)):
                kept = pl.ds(pl.multiple_of((j * ML + m) * NY, 8), NY)
                if h < HALVES - 1:
                    mid[kept, :] = stepped[:, tile(k)]
                else:
                    first, second = pair_up(mid[kept, :], stepped[:, tile(k)], lane128, VH)
                    q_v[m, :, tile(2 * j)] = first
                    q_v[m, :, tile(2 * j + 1)] = second
            return carry

        lax.fori_loop(0, ML // 2, one, 0, unroll=3)

    def inner(t):
        top, rest = split2(q_v[:, :, tile(t)].reshape(ML * NY, LANES))
        tn = (((0,), (0,)), ((), ()))
        return lax.dot_general(
            top, jnp.concatenate([top, rest], axis=1), tn, preferred_element_type=F32
        )

    stores = [
        pltpu.make_async_copy(q_v.at[:, :, cut(j)], stepped_hbm.at[:, :, cut(j)], out_sems.at[j])
        for j in range(TILES)
    ]
    drain(land, 0, PIECE, rr.at[0])
    for j in range(TILES):
        solve(0, j)
    whole = jnp.zeros((LANES, wide), F32)
    for j in range(TILES):
        if j == 0:
            drain(land, SPAN, EARLY, rr.at[1])
        if j == TILES - 1:
            drain(land, SPAN, PIECE - EARLY, rr.at[2])
        solve(1, j)
        stores[j].start()
        whole += inner(2 * j) + inner(2 * j + 1)

    cross = whole[:, LANES:]
    whole = whole[:, :LANES] + cross + cross.T
    own = whole[:NV]
    for low in range(1, BLO):
        own += pltpu.roll(whole[NV * low : NV * (low + 1)], LANES - NV * low, 1)
    lane32 = lax.broadcasted_iota(jnp.int32, (NV, LANES), 1)
    own = jnp.where(lane32 < NV, own, 0.0)
    packed = own[:8]
    for k in range(1, NV // 8):
        packed += pltpu.roll(own[8 * k : 8 * k + 8], NV * k, 1)

    gram_own[...] = packed
    gram_col[c] = packed

    def send_col(k, carry):
        pltpu.make_async_remote_copy(
            gram_own, gram_col.at[c], cs, cr,
            device_id=(r, lax.rem(c + k, NC)), device_id_type=MESH,
        ).start()
        return carry

    lax.fori_loop(1, NC, send_col, 0)
    part = gram_col.at[pl.ds(0, NC - 1)]
    pltpu.make_async_copy(part, part, cr).wait()
    total = gram_col[0]
    for k in range(1, NC):
        total += gram_col[k]
    gram_row_own[...] = total
    gram_row[r] = total

    def send_row(k, carry):
        pltpu.make_async_remote_copy(
            gram_row_own, gram_row.at[r], ws, wr,
            device_id=(lax.rem(r + k, NR), c), device_id_type=MESH,
        ).start()
        return carry

    lax.fori_loop(1, NR, send_row, 0)
    part = gram_row.at[pl.ds(0, NR - 1)]
    pltpu.make_async_copy(part, part, wr).wait()
    total = gram_row[0]
    for k in range(1, NR):
        total += gram_row[k]

    gram_ref[...] = total

    drain(base_send, 0, BASE, bs)
    drain(send, 0, HALVES * PIECE, rs)
    part = gram_col.at[pl.ds(0, NC - 1)]
    pltpu.make_async_copy(part, part, cs).wait()
    part = gram_row.at[pl.ds(0, NR - 1)]
    pltpu.make_async_copy(part, part, ws).wait()
    for copy in stores:
        copy.wait()


def eliminate(total):
    lane = lax.broadcasted_iota(jnp.int32, (NV, LANES), 1)
    row = lax.broadcasted_iota(jnp.int32, (NV, LANES), 0)
    gram = jnp.concatenate(
        [total] + [pltpu.roll(total, LANES - NV * k, 1) for k in range(1, NV // 8)], axis=0
    )
    gram = gram / float(NX * NY * NZ)
    work = jnp.where(lane < NV, gram, jnp.where(lane == row + NV, 1.0, 0.0))
    for k in range(NV - 1):
        pivot_row = work[k : k + 1, :]
        factor = work[:, k : k + 1] / work[k : k + 1, k : k + 1]
        work = work - jnp.where(row > k, factor, 0.0) * pivot_row
    on_diagonal = jnp.where(lane == row, work, 0.0)
    scale = 1.0 / jnp.sqrt(jnp.sum(on_diagonal, axis=1, keepdims=True))
    keep = (lane >= NV) & (lane < 2 * NV)
    inverse = pltpu.roll(jnp.where(keep, work, 0.0), LANES - NV, 1) * scale
    inverse = jnp.concatenate(
        [inverse] + [pltpu.roll(inverse, NV * k, 1) for k in range(1, BLO)], axis=0
    )
    diagonal = jnp.sum(on_diagonal, axis=0, keepdims=True)
    return inverse, 0.5 * jnp.log(diagonal[:, :NV])


def turn_kernel(
    stepped_hbm, gram_hbm, out_hbm, growth_out, x_v, y_v, gram_v, in_sems, out_sems, gram_sem,
):
    def load(t):
        at = pl.ds(pl.multiple_of(t * LANES, LANES), LANES)
        return pltpu.make_async_copy(stepped_hbm.at[:, :, at], x_v.at[t], in_sems.at[t])

    def store(t):
        at = pl.ds(pl.multiple_of(t * LANES, LANES), LANES)
        return pltpu.make_async_copy(y_v.at[t], out_hbm.at[:, :, at], out_sems.at[t])

    count = x_v.shape[0]
    gram_copy = pltpu.make_async_copy(gram_hbm, gram_v, gram_sem)
    gram_copy.start()
    for t in range(count):
        load(t).start()
    gram_copy.wait()
    inverse, growth_out[...] = eliminate(gram_v[...])
    right = jnp.concatenate(split2(inverse.T), axis=1)
    right = jnp.concatenate([right, right], axis=0)

    def one(t, carry):
        load(t).wait()
        rows = x_v[t].reshape(ML * NY, LANES)
        both = mm(jnp.concatenate(split2(rows), axis=1), right)
        y_v[t] = (both[:, :LANES] + both[:, LANES:]).reshape(ML, NY, LANES)
        store(t).start()
        return carry

    lax.fori_loop(0, count, one, 0)
    for t in range(count):
        store(t).wait()


def body(tangents, base_flow, mode_mask, decay_rates, to_eigen, from_eigen):
    constants = [jnp.asarray(t) for t in tables()]
    inputs = [
        tangents, jnp.transpose(base_flow, (0, 2, 1)), mode_mask, decay_rates.reshape(1, NY),
        to_eigen, from_eigen,
    ] + constants
    vmem = pl.BlockSpec(memory_space=pltpu.VMEM)
    anywhere = pl.BlockSpec(memory_space=pl.ANY)
    dma = pltpu.SemaphoreType.DMA
    field = pltpu.VMEM((HALVES * SPAN, LANES), F32)
    stepped, gram = pl.pallas_call(
        step_kernel,
        out_shape=(
            jax.ShapeDtypeStruct(tangents.shape, F32),
            jax.ShapeDtypeStruct((8, LANES), F32),
        ),
        in_specs=[anywhere] * len(inputs),
        out_specs=(anywhere, vmem),
        scratch_shapes=[
            pltpu.VMEM(tangents.shape, F32), field, field,
            pltpu.VMEM((HI * NX, LANES), F32),
            pltpu.VMEM((HI // QUAD, NZ, QUAD * LANES), F32), field,
            pltpu.VMEM(inputs[1].shape, F32),
            pltpu.VMEM((ND * BASE, LANES), F32),
            pltpu.VMEM((ND * BASE, LANES), F32),
            pltpu.VMEM(mode_mask.shape, jnp.int32),
            pltpu.VMEM((16 * TILES, LANES), F32),
            pltpu.VMEM((1, NY), F32),
            pltpu.VMEM((NY, NY), F32),
            pltpu.VMEM((NY, NY), F32),
            pltpu.VMEM((2 * NY, 2 * NY), BF16),
            pltpu.VMEM((2 * NY, 2 * NY), BF16),
        ]
        + [pltpu.VMEM(t.shape, t.dtype) for t in constants]
        + [
            pltpu.VMEM((8, LANES), F32),
            pltpu.VMEM((NC, 8, LANES), F32),
            pltpu.VMEM((8, LANES), F32),
            pltpu.VMEM((NR, 8, LANES), F32),
            dma((TILES,)), dma((len(inputs) - 1,)), dma((TILES,)),
            dma((HALVES,)), dma((HALVES,)), dma((3,)),
        ]
        + [dma] * 7,
        compiler_params=pltpu.CompilerParams(
            collective_id=0, has_side_effects=True, vmem_limit_bytes=60 * 2**20
        ),
        name="step",
    )(*inputs)

    tiles = tangents.shape[2] // LANES
    vectors, growth = pl.pallas_call(
        turn_kernel,
        out_shape=(
            jax.ShapeDtypeStruct(tangents.shape, F32),
            jax.ShapeDtypeStruct((1, NV), F32),
        ),
        in_specs=[pl.BlockSpec(memory_space=pltpu.HBM)] * 2,
        out_specs=(anywhere, vmem),
        scratch_shapes=[
            pltpu.VMEM((tiles, ML, NY, LANES), F32),
            pltpu.VMEM((tiles, ML, NY, LANES), F32),
            pltpu.VMEM((8, LANES), F32),
            dma((tiles,)), dma((tiles,)), dma,
        ],
        compiler_params=pltpu.CompilerParams(vmem_limit_bytes=60 * 2**20),
        name="turn",
    )(stepped, gram)
    return vectors, growth.reshape(NV)


def solution(mesh):
    placed = (P("row", None, "col"), P("row", None, "col"), P("row", "col"), P(), P(), P())
    return jax.shard_map(
        body, mesh=mesh, in_specs=placed, out_specs=(P("row", None, "col"), P()), check_vma=False
    )
```

```python
import functools
import math

import jax
import jax.numpy as jnp
import numpy as np
from jax import lax
from jax.experimental import pallas as pl
from jax.experimental.pallas import tpu as pltpu
from jax.sharding import PartitionSpec as P

MESH = pl.DeviceIdType.MESH
F32 = jnp.float32
BF16 = jnp.bfloat16
STEP_COEF = 10.0
VISCOSITY = 0.01
ALPHA_X = 0.5
BETA_Z = 1.0

NX = 192
NY = 128
NZ = 192
NV = 32
NR, NC = 16, 8
ND = NR * NC
ML = NX // NR
NL = NZ // NC
LANES = 128
HALVES = 2
VH = NV // HALVES
LO = LANES // VH
HI = NZ // LO
TILES = HI // NC
PIECE = ML * TILES
PITCH = 40
SPAN = ND * PITCH
EARLY = 24
BLO = LANES // NV
BHI = NX // BLO
BASE = ML // BLO
QUAD = 4
HOP = 101


def synthesis(n):
    point = np.arange(n)[:, None]
    mode = np.arange(n)[None, :]
    wave = np.where(mode <= n // 2, mode, mode - n // 2)
    angle = (point * wave % n) * (2.0 * math.pi / n)
    return np.where(mode <= n // 2, np.cos(angle), np.sin(angle))


def analysis(n):
    mode = np.arange(n)
    weight = np.where((mode == 0) | (mode == n // 2), 1.0 / n, 2.0 / n)
    return weight[:, None] * synthesis(n).T


def derivative_analysis(n):
    derivative = np.zeros((n, n))
    k = np.arange(1, n // 2)
    derivative[k, n // 2 + k] = k
    derivative[n // 2 + k, k] = -k
    return -ALPHA_X * (derivative @ analysis(n))


def waves(n):
    mode = np.arange(n)
    return np.where(mode <= n // 2, mode, mode - n // 2).astype(np.float32)


def halves(table):
    table = np.asarray(table, np.float32)
    top = table.astype(BF16)
    rest = (table - top.astype(np.float32)).astype(BF16)
    return np.concatenate([top, rest], axis=0)


def mode_slots(tail_first):
    slots = -np.ones((NR, 16), np.int64)
    for r in range(NR):
        for k in range(16):
            if tail_first:
                if k >= 8:
                    slots[r, k] = ML * r + k - 8
                elif k >= 4:
                    slots[r, k] = ML * r + 8 + k - 4
            elif k < ML:
                slots[r, k] = ML * r + k
    return slots.reshape(-1)


def spanwise_of(block):
    return block // 2 + 4 * (block % 2)


def tables():
    low, high = np.arange(LO)[:, None], np.arange(HI)[None, :]
    modes = (LO * high + spanwise_of(low)).reshape(-1)
    points = (LO * high + low).reshape(-1)
    sx, sz = synthesis(NX), synthesis(NZ)
    gx, az = derivative_analysis(NX), analysis(NZ)
    forward, backward = [], []
    for tail_first in (False, True):
        slots = mode_slots(tail_first)
        live = slots >= 0
        w = np.zeros((NX, NR * 16))
        w[:, live] = sx[:, slots[live]]
        forward.append(halves(w))
        g = np.zeros((NR * 16, NX))
        g[live] = gx[slots[live]][:, points]
        backward.append(halves(g))
    base_x = np.concatenate([sx[:, k::BLO] for k in range(BLO)], axis=0)
    top, rest = np.split(halves(base_x), 2)
    base_x3 = np.concatenate([top, rest, top], axis=1)
    base_z = np.zeros((NZ, NC, BLO, NV))
    base_z[:, :, :, :NL] = sz.reshape(NZ, NC, 1, NL)
    return (
        np.stack(forward),
        np.stack(backward),
        halves(sz[:, modes]),
        halves(az[modes]),
        base_x3,
        halves(base_z.reshape(NZ, NC * LANES)),
    )


def split2(x):
    top = x.astype(BF16)
    return top, (x - top.astype(F32)).astype(BF16)


def mm(a, b):
    return jnp.dot(a, b, preferred_element_type=F32)


def mm3(table, x):
    rows = table.shape[0] // 2
    top, rest = split2(x)
    both = mm(table, top)
    return both[:rows] + both[rows:] + mm(table[:rows], rest)


def even_blocks(lane, width):
    return (lane // width) % 2 == 0


def pair_up(x, y, lane, width):
    mask = even_blocks(lane, width)
    return (
        jnp.where(mask, x, pltpu.roll(y, width, 1)),
        jnp.where(mask, pltpu.roll(x, LANES - width, 1), y),
    )


def swap_blocks(parts, lane):
    parts = list(parts)
    bit = LO // 2
    while bit:
        for k in range(LO):
            if not k & bit:
                parts[k], parts[k | bit] = pair_up(parts[k], parts[k | bit], lane, VH * bit)
        bit //= 2
    return parts


def farthest_first(side):
    offsets = [
        (y, x, z, core)
        for y in range(side) for x in range(side) for z in range(side) for core in range(2)
    ]
    hops = lambda offset: sum(min(k, side - k) for k in offset[:3])
    return sorted(offsets[1:], key=hops, reverse=True)


def step_kernel(
    q_hbm, base_hbm, mask_hbm, decay_hbm, to_hbm, from_hbm,
    fwd_hbm, bwd_hbm, sz_hbm, az_hbm, bx_hbm, bz_hbm,
    stepped_hbm, gram_ref,
    q_v, send, recv, mid, speed, land,
    base_v, base_send, base_recv, mask_v, mask_w, decay_v, to_v, from_v, to_s, from_s,
    fwd_v, bwd_v, sz_v, az_v, bx_v, bz_v,
    gram_own, gram_col, gram_row_own, gram_row,
    q_sems, in_sems, out_sems, fs, fr, rr,
    bs, br, rs, cs, cr, ws, wr,
):
    r = lax.axis_index("row")
    c = lax.axis_index("col")
    me = r * NC + c
    my_slot = c * NR + r
    wide = 2 * LANES

    def cut(j):
        return slice(wide * j, wide * (j + 1))

    def tile(t):
        return slice(LANES * t, LANES * (t + 1))

    small = [
        pltpu.make_async_copy(src, dst, in_sems.at[k])
        for k, (src, dst) in enumerate(
            [
                (base_hbm, base_v), (bx_hbm, bx_v), (bz_hbm, bz_v), (fwd_hbm, fwd_v),
                (sz_hbm, sz_v), (az_hbm, az_v), (bwd_hbm, bwd_v), (mask_hbm, mask_v),
                (decay_hbm, decay_v), (to_hbm, to_v), (from_hbm, from_v),
            ]
        )
    ]
    loads = [
        pltpu.make_async_copy(q_hbm.at[:, :, cut(j)], q_v.at[:, :, cut(j)], q_sems.at[j])
        for j in range(TILES)
    ]
    small[0].start()
    for copy in loads:
        copy.start()
    for copy in small[1:]:
        copy.start()

    def partner(k):
        off = lax.rem(k * HOP, ND)
        return lax.rem(r + off // NC, NR), lax.rem(c + lax.rem(off, NC), NC)

    barrier = pltpu.get_barrier_semaphore()

    side = 4
    ys = [lax.rem(r // side + k, side) * side for k in range(side)]
    xs = [lax.rem(lax.rem(r, side) + k, side) for k in range(side)]
    zs = [lax.rem(c // 2 + k, side) * 2 for k in range(side)]
    cores = [lax.rem(c, 2), 1 - lax.rem(c, 2)]
    for y, x, z, core in farthest_first(side):
        pl.semaphore_signal(
            barrier, inc=1, device_id=(ys[y] + xs[x], zs[z] + cores[core]), device_id_type=MESH
        )

    def row_of(j, m):
        return (m, jnp.where(m < 8, 16 + m, 4 + m), 24 + m)[j]

    def half_of(first, second, lane, h):
        return pair_up(first, second, lane, VH)[h]

    lane8 = lax.broadcasted_iota(jnp.int32, (8, LANES), 1)

    def pack(h):
        def one(m, carry):
            for j in range(TILES):
                for t in range(NY // 8):
                    rows = slice(8 * t, 8 * t + 8)
                    send[pl.ds(h * SPAN + 8 * t * PITCH + row_of(j, m), 8, stride=PITCH), :] = half_of(
                        q_v[m, rows, tile(2 * j)], q_v[m, rows, tile(2 * j + 1)], lane8, h
                    )
            return carry

        lax.fori_loop(0, ML, one, 0)

    def send_forward(h):
        def one(k, carry):
            r2, c2 = partner(k)
            pltpu.make_async_remote_copy(
                send.at[pl.ds(h * SPAN + (r2 * NC + c2) * PITCH, PIECE)],
                recv.at[pl.ds(h * SPAN + my_slot * PITCH, PIECE)],
                fs.at[h], fr.at[h], device_id=(r2, c2), device_id_type=MESH,
            ).start()
            return carry

        lax.fori_loop(1, ND, one, 0)

    def send_base(k, carry):
        r2, c2 = partner(k)
        pltpu.make_async_remote_copy(
            base_send.at[pl.ds((r2 * NC + c2) * BASE, BASE)],
            base_recv.at[pl.ds(my_slot * BASE, BASE)],
            bs, br, device_id=(r2, c2), device_id_type=MESH,
        ).start()
        return carry

    def keep_own(dst, to, h):
        dst[pl.ds(pl.multiple_of(h * SPAN + to * PITCH, 8), PIECE), :] = send[
            pl.ds(pl.multiple_of(h * SPAN + me * PITCH, 8), PIECE), :
        ]

    for copy in loads:
        copy.wait()
    pack(0)

    def clear(k, carry):
        recv[pl.ds(PITCH * k + PIECE, PITCH - PIECE), :] = jnp.zeros((PITCH - PIECE, LANES), F32)
        return carry

    lax.fori_loop(0, HALVES * ND, clear, 0, unroll=4)
    pl.semaphore_wait(barrier, ND - 1)
    send_forward(0)

    small[0].wait()
    gap = jnp.zeros((NV - NL, NY), F32)
    for high in range(BASE):
        stack = []
        for low in range(BLO):
            stack += [base_v[high * BLO + low], gap]
        turned = jnp.concatenate(stack, axis=0).T
        for t in range(NY // 8):
            base_send[pl.ds(8 * t * BASE + high, 8, stride=BASE), :] = turned[8 * t : 8 * t + 8]

    lax.fori_loop(1, ND, send_base, 0)
    pack(1)
    send_forward(1)
    base_recv[pl.ds(my_slot * BASE, BASE), :] = base_send[pl.ds(me * BASE, BASE), :]
    for h in range(HALVES):
        keep_own(recv, my_slot, h)

    def drain(ref, first, rows, sem):
        part = ref.at[pl.ds(first, (ND - 1) * rows)]
        pltpu.make_async_copy(part, part, sem).wait()

    for copy in small[1:]:
        copy.wait()
    for src, dst in ((to_v, to_s), (from_v, from_s)):
        both = jnp.concatenate(split2(src[...]), axis=0)
        dst[...] = jnp.concatenate([both, both], axis=1)
    spot = lax.broadcasted_iota(jnp.int32, (NL, TILES * LANES), 1) // VH
    column = LO * (spot // LO) + spanwise_of(lax.rem(spot, LO))
    pick = lax.broadcasted_iota(jnp.int32, (NL, TILES * LANES), 0) == column
    retained = mm(mask_v[...].astype(F32).astype(BF16), pick.astype(F32).astype(BF16))
    for j in range(TILES):
        mask_w[16 * j : 16 * j + ML, :] = retained[:, tile(j)]

    drain(base_recv, 0, BASE, br)
    block = (lax.broadcasted_iota(jnp.int32, (NX, wide), 1) // NV) % BLO
    speed_t = jnp.zeros((NZ, NX), F32)
    nt = (((1,), (1,)), ((), ()))
    for pair in range(NC // 2):
        field = jnp.concatenate(
            [base_recv[(2 * pair + h) * BHI : (2 * pair + h + 1) * BHI, :] for h in range(2)],
            axis=1,
        )
        top, rest = split2(field)
        out = mm(bx_v[...], jnp.concatenate([top, top, rest], axis=0))
        half = jnp.zeros((NX, wide), F32)
        for low in range(BLO):
            half = jnp.where(block == low, out[low * NX : (low + 1) * NX], half)
        top, rest = split2(half)
        table = bz_v[:, cut(pair)]
        both = lax.dot_general(table, top, nt, preferred_element_type=F32)
        speed_t += both[:NZ] + both[NZ:] + lax.dot_general(
            table[:NZ], rest, nt, preferred_element_type=F32
        )
    speed_parts = jnp.concatenate(split2(speed_t), axis=0)
    spread_shape = (NX, QUAD * LANES)
    point = lax.broadcasted_iota(jnp.int32, spread_shape, 0)
    spot_x = lax.broadcasted_iota(jnp.int32, spread_shape, 1) // VH

    def spread(i, carry):
        pick = (point == QUAD * LO * i + spot_x).astype(F32).astype(BF16)
        both = mm(speed_parts, pick)
        speed[i] = both[:NZ] + both[NZ:]
        return carry

    lax.fori_loop(0, HI // QUAD, spread, 0)

    types = ((0, (0, 2)), (1, (1,)))
    first_row = (0, 8, 24)

    def x_forward(h):
        def one(i, carry):
            for e, tiles in types:
                at = [(2 * i + k, j) for k in range(2) for j in tiles]
                sides = []
                for c2, j in at:
                    base = h * SPAN + c2 * (NR * PITCH) + first_row[j]
                    sides.append(
                        jnp.concatenate(
                            [
                                recv[pl.ds(pl.multiple_of(base + PITCH * k, 8), 16), :]
                                for k in range(NR)
                            ],
                            axis=0,
                        )
                    )
                out = mm3(fwd_v[e], jnp.concatenate(sides, axis=1))
                for k, (c2, j) in enumerate(at):
                    to = (TILES * c2 + j) * NX
                    mid[pl.ds(pl.multiple_of(to, 8), NX), :] = out[:, tile(k)]
            return carry

        lax.fori_loop(0, NC // 2, one, 0, unroll=2)

    lane24 = lax.broadcasted_iota(jnp.int32, (HI, LANES), 1)

    def gathered(ref, first):
        return jnp.concatenate(
            [ref[pl.ds(8 * a * NX + first, 8, stride=NX), :] for a in range(HI // 8)], axis=0
        )

    def swapped(ref, starts):
        parts = [gathered(ref, first) for first in starts]
        return jnp.concatenate(swap_blocks(parts, lane24), axis=0)

    def z_both(h):
        def one(i, carry):
            sides = [
                swapped(mid, [(QUAD * i + k) * LO + low for low in range(LO)]) for k in range(QUAD)
            ]
            physical = mm3(sz_v[...], jnp.concatenate(sides, axis=1))
            out = mm3(az_v[...], physical * speed[i])
            for k in range(QUAD):
                to = h * SPAN + (QUAD * i + k) * NX
                recv[pl.ds(pl.multiple_of(to, 8), NX), :] = out[:, tile(k)]
            return carry

        lax.fori_loop(0, HI // QUAD, one, 0, unroll=2)

    def x_backward(h):
        def one(i, carry):
            done = {}
            for e, tiles in types:
                at = [(k, j) for k in range(2) for j in tiles]
                sides = []
                for k, j in at:
                    high = TILES * (2 * i + k) + j
                    sides.append(swapped(recv, [h * SPAN + low * HI + high for low in range(LO)]))
                out = mm3(bwd_v[e], jnp.concatenate(sides, axis=1))
                for k, key in enumerate(at):
                    done[key] = out[:, tile(k)]
            for k in range(2):
                for r2 in range(NR):
                    t0, t1, t2 = (done[k, j][16 * r2 : 16 * r2 + 16] for j in range(TILES))
                    to = h * SPAN + (r2 * NC + 2 * i + k) * PITCH
                    send[pl.ds(pl.multiple_of(to, 8), PITCH), :] = jnp.concatenate(
                        [t0[:8], t0[8:] + t1[:8], t1[8:], t2], axis=0
                    )
            return carry

        lax.fori_loop(0, NC // 2, one, 0)

    def send_back(h, first, rows, sem):
        def one(k, carry):
            r2, c2 = partner(k)
            pltpu.make_async_remote_copy(
                send.at[pl.ds(h * SPAN + (r2 * NC + c2) * PITCH + first, rows)],
                land.at[pl.ds(h * SPAN + me * PITCH + first, rows)],
                rs, sem, device_id=(r2, c2), device_id_type=MESH,
            ).start()
            return carry

        lax.fori_loop(1, ND, one, 0)

    for h in range(HALVES):
        drain(recv, h * SPAN, PIECE, fr.at[h])
        x_forward(h)
        z_both(h)
        drain(send, h * SPAN, PIECE, fs.at[h])
        x_backward(h)
        if h < HALVES - 1:
            send_back(h, 0, PIECE, rr.at[0])
        else:
            send_back(h, 0, EARLY, rr.at[1])
            send_back(h, EARLY, PIECE - EARLY, rr.at[2])
        keep_own(land, me, h)

    decay = jnp.broadcast_to(decay_v[...], (NY, NY)).T
    decay = jnp.concatenate([decay, decay], axis=1)
    lane128 = lax.broadcasted_iota(jnp.int32, (NY, LANES), 1)
    spot = lax.broadcasted_iota(jnp.int32, (1, LANES), 1) // VH

    def wave_of(mode, count):
        return jnp.where(mode <= count // 2, mode, mode - count // 2).astype(F32)

    def solve(h, j):
        wave_z = BETA_Z * wave_of(c * NL + LO * j + spanwise_of(spot), NZ)
        square_z = wave_z * wave_z

        def one(i, carry):
            right, squares = [], []
            for m in (2 * i, 2 * i + 1):
                nonlinear = jnp.concatenate(
                    [
                        land[pl.ds(h * SPAN + 8 * t * PITCH + row_of(j, m), 8, stride=PITCH), :]
                        for t in range(NY // 8)
                    ],
                    axis=0,
                )
                field = half_of(q_v[m, :, tile(2 * j)], q_v[m, :, tile(2 * j + 1)], lane128, h)
                right.append(STEP_COEF * field + nonlinear * mask_w[pl.ds(16 * j + m, 1), :])
                wave_x = ALPHA_X * wave_of(r * ML + m, NX)
                squares.append(wave_x * wave_x + square_z)
            right = jnp.concatenate(right, axis=1)
            both = mm(to_s[...], jnp.concatenate(split2(right), axis=0))
            divisor = (STEP_COEF + VISCOSITY * jnp.concatenate(squares, axis=1)) + decay
            eigen = (both[:NY] + both[NY:]) / divisor
            both = mm(from_s[...], jnp.concatenate(split2(eigen), axis=0))
            stepped = both[:NY] + both[NY:]
            for k, m in enumerate((2 * i, 2 * i + 1)):
                kept = pl.ds(pl.multiple_of((j * ML + m) * NY, 8), NY)
                if h < HALVES - 1:
                    mid[kept, :] = stepped[:, tile(k)]
                else:
                    first, second = pair_up(mid[kept, :], stepped[:, tile(k)], lane128, VH)
                    q_v[m, :, tile(2 * j)] = first
                    q_v[m, :, tile(2 * j + 1)] = second
            return carry

        lax.fori_loop(0, ML // 2, one, 0, unroll=3)

    def inner(t):
        top, rest = split2(q_v[:, :, tile(t)].reshape(ML * NY, LANES))
        tn = (((0,), (0,)), ((), ()))
        return lax.dot_general(
            top, jnp.concatenate([top, rest], axis=1), tn, preferred_element_type=F32
        )

    stores = [
        pltpu.make_async_copy(q_v.at[:, :, cut(j)], stepped_hbm.at[:, :, cut(j)], out_sems.at[j])
        for j in range(TILES)
    ]
    drain(land, 0, PIECE, rr.at[0])
    for j in range(TILES):
        solve(0, j)
    whole = jnp.zeros((LANES, wide), F32)
    for j in range(TILES):
        if j == 0:
            drain(land, SPAN, EARLY, rr.at[1])
        if j == TILES - 1:
            drain(land, SPAN, PIECE - EARLY, rr.at[2])
        solve(1, j)
        stores[j].start()
        whole += inner(2 * j) + inner(2 * j + 1)

    cross = whole[:, LANES:]
    whole = whole[:, :LANES] + cross + cross.T
    own = whole[:NV]
    for low in range(1, BLO):
        own += pltpu.roll(whole[NV * low : NV * (low + 1)], LANES - NV * low, 1)
    lane32 = lax.broadcasted_iota(jnp.int32, (NV, LANES), 1)
    own = jnp.where(lane32 < NV, own, 0.0)
    packed = own[:8]
    for k in range(1, NV // 8):
        packed += pltpu.roll(own[8 * k : 8 * k + 8], NV * k, 1)

    gram_own[...] = packed
    gram_col[c] = packed

    def send_col(k, carry):
        pltpu.make_async_remote_copy(
            gram_own, gram_col.at[c], cs, cr,
            device_id=(r, lax.rem(c + k, NC)), device_id_type=MESH,
        ).start()
        return carry

    lax.fori_loop(1, NC, send_col, 0)
    part = gram_col.at[pl.ds(0, NC - 1)]
    pltpu.make_async_copy(part, part, cr).wait()
    total = gram_col[0]
    for k in range(1, NC):
        total += gram_col[k]
    gram_row_own[...] = total
    gram_row[r] = total

    def send_row(k, carry):
        pltpu.make_async_remote_copy(
            gram_row_own, gram_row.at[r], ws, wr,
            device_id=(lax.rem(r + k, NR), c), device_id_type=MESH,
        ).start()
        return carry

    lax.fori_loop(1, NR, send_row, 0)
    part = gram_row.at[pl.ds(0, NR - 1)]
    pltpu.make_async_copy(part, part, wr).wait()
    total = gram_row[0]
    for k in range(1, NR):
        total += gram_row[k]

    gram_ref[...] = total

    drain(base_send, 0, BASE, bs)
    drain(send, 0, HALVES * PIECE, rs)
    part = gram_col.at[pl.ds(0, NC - 1)]
    pltpu.make_async_copy(part, part, cs).wait()
    part = gram_row.at[pl.ds(0, NR - 1)]
    pltpu.make_async_copy(part, part, ws).wait()
    for copy in stores:
        copy.wait()


def eliminate(total):
    lane = lax.broadcasted_iota(jnp.int32, (NV, LANES), 1)
    row = lax.broadcasted_iota(jnp.int32, (NV, LANES), 0)
    gram = jnp.concatenate(
        [total] + [pltpu.roll(total, LANES - NV * k, 1) for k in range(1, NV // 8)], axis=0
    )
    gram = gram / float(NX * NY * NZ)
    work = jnp.where(lane < NV, gram, jnp.where(lane == row + NV, 1.0, 0.0))
    for k in range(NV - 1):
        pivot_row = work[k : k + 1, :]
        factor = work[:, k : k + 1] / work[k : k + 1, k : k + 1]
        work = work - jnp.where(row > k, factor, 0.0) * pivot_row
    on_diagonal = jnp.where(lane == row, work, 0.0)
    scale = 1.0 / jnp.sqrt(jnp.sum(on_diagonal, axis=1, keepdims=True))
    keep = (lane >= NV) & (lane < 2 * NV)
    inverse = pltpu.roll(jnp.where(keep, work, 0.0), LANES - NV, 1) * scale
    inverse = jnp.concatenate(
        [inverse] + [pltpu.roll(inverse, NV * k, 1) for k in range(1, BLO)], axis=0
    )
    diagonal = jnp.sum(on_diagonal, axis=0, keepdims=True)
    return inverse, 0.5 * jnp.log(diagonal[:, :NV])


def turn_kernel(
    stepped_hbm, gram_hbm, out_hbm, growth_out, x_v, y_v, gram_v, in_sems, out_sems, gram_sem,
):
    def load(t):
        at = pl.ds(pl.multiple_of(t * LANES, LANES), LANES)
        return pltpu.make_async_copy(stepped_hbm.at[:, :, at], x_v.at[t], in_sems.at[t])

    def store(t):
        at = pl.ds(pl.multiple_of(t * LANES, LANES), LANES)
        return pltpu.make_async_copy(y_v.at[t], out_hbm.at[:, :, at], out_sems.at[t])

    count = x_v.shape[0]
    gram_copy = pltpu.make_async_copy(gram_hbm, gram_v, gram_sem)
    gram_copy.start()
    for t in range(count):
        load(t).start()
    gram_copy.wait()
    inverse, growth_out[...] = eliminate(gram_v[...])
    right = jnp.concatenate(split2(inverse.T), axis=1)
    right = jnp.concatenate([right, right], axis=0)

    def one(t, carry):
        load(t).wait()
        rows = x_v[t].reshape(ML * NY, LANES)
        both = mm(jnp.concatenate(split2(rows), axis=1), right)
        y_v[t] = (both[:, :LANES] + both[:, LANES:]).reshape(ML, NY, LANES)
        store(t).start()
        return carry

    lax.fori_loop(0, count, one, 0)
    for t in range(count):
        store(t).wait()


def body(tangents, base_flow, mode_mask, decay_rates, to_eigen, from_eigen):
    constants = [jnp.asarray(t) for t in tables()]
    inputs = [
        tangents, jnp.transpose(base_flow, (0, 2, 1)), mode_mask, decay_rates.reshape(1, NY),
        to_eigen, from_eigen,
    ] + constants
    vmem = pl.BlockSpec(memory_space=pltpu.VMEM)
    anywhere = pl.BlockSpec(memory_space=pl.ANY)
    dma = pltpu.SemaphoreType.DMA
    field = pltpu.VMEM((HALVES * SPAN, LANES), F32)
    stepped, gram = pl.pallas_call(
        step_kernel,
        out_shape=(
            jax.ShapeDtypeStruct(tangents.shape, F32),
            jax.ShapeDtypeStruct((8, LANES), F32),
        ),
        in_specs=[anywhere] * len(inputs),
        out_specs=(anywhere, vmem),
        scratch_shapes=[
            pltpu.VMEM(tangents.shape, F32), field, field,
            pltpu.VMEM((HI * NX, LANES), F32),
            pltpu.VMEM((HI // QUAD, NZ, QUAD * LANES), F32), field,
            pltpu.VMEM(inputs[1].shape, F32),
            pltpu.VMEM((ND * BASE, LANES), F32),
            pltpu.VMEM((ND * BASE, LANES), F32),
            pltpu.VMEM(mode_mask.shape, jnp.int32),
            pltpu.VMEM((16 * TILES, LANES), F32),
            pltpu.VMEM((1, NY), F32),
            pltpu.VMEM((NY, NY), F32),
            pltpu.VMEM((NY, NY), F32),
            pltpu.VMEM((2 * NY, 2 * NY), BF16),
            pltpu.VMEM((2 * NY, 2 * NY), BF16),
        ]
        + [pltpu.VMEM(t.shape, t.dtype) for t in constants]
        + [
            pltpu.VMEM((8, LANES), F32),
            pltpu.VMEM((NC, 8, LANES), F32),
            pltpu.VMEM((8, LANES), F32),
            pltpu.VMEM((NR, 8, LANES), F32),
            dma((TILES,)), dma((len(inputs) - 1,)), dma((TILES,)),
            dma((HALVES,)), dma((HALVES,)), dma((3,)),
        ]
        + [dma] * 7,
        compiler_params=pltpu.CompilerParams(
            collective_id=0, has_side_effects=True, vmem_limit_bytes=60 * 2**20
        ),
        name="step",
    )(*inputs)

    tiles = tangents.shape[2] // LANES
    vectors, growth = pl.pallas_call(
        turn_kernel,
        out_shape=(
            jax.ShapeDtypeStruct(tangents.shape, F32),
            jax.ShapeDtypeStruct((1, NV), F32),
        ),
        in_specs=[pl.BlockSpec(memory_space=pltpu.HBM)] * 2,
        out_specs=(anywhere, vmem),
        scratch_shapes=[
            pltpu.VMEM((tiles, ML, NY, LANES), F32),
            pltpu.VMEM((tiles, ML, NY, LANES), F32),
            pltpu.VMEM((8, LANES), F32),
            dma((tiles,)), dma((tiles,)), dma,
        ],
        compiler_params=pltpu.CompilerParams(vmem_limit_bytes=60 * 2**20),
        name="turn",
    )(stepped, gram)
    return vectors, growth.reshape(NV)


def solution(mesh):
    placed = (P("row", None, "col"), P("row", None, "col"), P("row", "col"), P(), P(), P())
    return jax.shard_map(
        body, mesh=mesh, in_specs=placed, out_specs=(P("row", None, "col"), P()), check_vma=False
    )
```
